256 devices in a mesh: role: 2 (over core), wide: 8 (over x_hi, y), tp: 16 (over z, x_lo).
Axes of the slice: x: 4 (x_hi: 2, x_lo: 2; x = x_hi * 2 + x_lo), y: 4, z: 8, core: 2. Of those that a mesh axis runs over, the one named last changes fastest.
Arguments:
- normed: bfloat16 [4096, 4096], P('wide', ('role', 'tp')), may hold values from -0.29882812 to 0.29882812
- queries: bfloat16 [4096, 4096], P('wide', 'tp'), may hold values from -4 to 4
- keys: bfloat16 [4096, 1024], P('wide'), may hold values from -4 to 4
- values: bfloat16 [4096, 1024], P('wide'), may hold values from -6 to 6
- attn_out: bfloat16 [4096, 4096], P('wide', 'tp'), may hold values from -0.29882812 to 0.29882812
- row_logsumexp: float32 [32, 4096], P('tp'), as said below
- out_grad: bfloat16 [4096, 4096], P('wide', ('role', 'tp')), may hold values from -6 to 6
- out_weight: bfloat16 [4096, 4096], P('tp'), may hold values from -0.09375 to 0.09375
- qkv_weight: bfloat16 [4096, 6144], P(('role', 'tp')), may hold values from -0.09375 to 0.09375
- documents: int32 [4096], replicated, may hold values from 0 to 2, as said below
- tasks: int32 [8, 16, 2], replicated, may hold values from -1 to 15, as said below
Outputs:
- normed_grad: bfloat16 [4096, 4096], P('wide', ('role', 'tp'))
- out_weight_grad: bfloat16 [4096, 4096], P('tp', ('role', 'wide'))
- qkv_weight_grad: bfloat16 [4096, 6144], P(('role', 'tp'), 'wide')
The draws below stay inside these ranges and needn't reach their ends.
Inputs may be any that keep to these rules, and one draw needn't show every extreme that they name: `documents`: document numbers never fall along the tokens, and every number from 0 to 2 is used. `tasks`: row s lists in its first slots the query blocks of server s, in [s, j, 0], followed by slots holding -1 in both places; every query block from 0 to 15 stands in exactly one slot of the table; [s, j, 1] is the block holding the first token of the document of the query block's first token. row_logsumexp[h, i] is the logarithm of the sum, over the tokens j that token i may attend, of exp(scores[h, i, j]) as computed from queries and keys.
All inputs are finite; a program needn't handle non-finite values.
Results may differ from the reference program's by a relative error of at most 0.018.
Values may be sent and summed in bfloat16 or wider, within the bound.
A program may use at most 128 MiB of HBM per device.

```python
import jax
import jax.numpy as jnp
from jax import lax

D = 4096
QUERY_HEADS = 32
KEY_VALUE_HEADS = 8
HEAD_SIZE = 128
DOCS = 3
QKV = 6144
QB = 256
WINDOW_TOKENS = 4096
SERVERS = 8


def layout(random_seed):
    block_count = WINDOW_TOKENS // QB
    cut_points = jax.random.permutation(jax.random.fold_in(random_seed, 11), WINDOW_TOKENS - 1)[:DOCS - 1] + 1
    positions = jnp.arange(WINDOW_TOKENS, dtype=jnp.int32)
    documents = jnp.sum((positions[:, None] >= cut_points[None, :]).astype(jnp.int32), axis=1).astype(jnp.int32)
    leading = documents[::QB]
    doc_starts = jnp.sum((documents[None, :] < leading[:, None]).astype(jnp.int32), axis=1)
    first_blocks = (doc_starts // QB).astype(jnp.int32)
    block_ids = jnp.arange(block_count, dtype=jnp.int32)
    tile_counts = block_ids - first_blocks + 1
    ranking = jnp.argsort(-(tile_counts * block_count + (block_count - 1 - block_ids)))

    def assign(number, carry):
        plan, server_load, filled = carry
        chosen = ranking[number]
        target = jnp.argmin(server_load)
        position = filled[target]
        plan = plan.at[target, position, 0].set(chosen)
        plan = plan.at[target, position, 1].set(first_blocks[chosen])
        return (plan, server_load.at[target].add(tile_counts[chosen]), filled.at[target].add(1))
    plan = jnp.full((SERVERS, block_count, 2), -1, jnp.int32)
    server_load = jnp.zeros((SERVERS,), jnp.int32)
    plan, server_load, filled = lax.fori_loop(0, block_count, assign, (plan, server_load, server_load))
    return (documents, plan)


def query_key(random_seed):
    query_noise = jax.random.normal(jax.random.fold_in(random_seed, 21), (WINDOW_TOKENS, QUERY_HEADS * HEAD_SIZE), jnp.float32)
    noise_key = jax.random.normal(jax.random.fold_in(random_seed, 22), (WINDOW_TOKENS, KEY_VALUE_HEADS * HEAD_SIZE), jnp.float32)
    return (jnp.clip(query_noise, -4.0, 4.0).astype(jnp.bfloat16), jnp.clip(noise_key, -4.0, 4.0).astype(jnp.bfloat16))


def draw_documents(key, part):
    return layout(jax.random.fold_in(key, 5))[0]


def draw_tasks(key, part):
    return layout(jax.random.fold_in(key, 5))[1]


def draw_queries(key, part):
    return query_key(jax.random.fold_in(key, 9))[0]


def draw_keys(key, part):
    return query_key(jax.random.fold_in(key, 9))[1]


def draw_row_logsumexp(key, part):
    queries, keys = query_key(jax.random.fold_in(key, 9))
    documents = layout(jax.random.fold_in(key, 5))[0]
    query_blocks = queries.astype(jnp.float32).reshape(WINDOW_TOKENS // QB, QB, QUERY_HEADS, HEAD_SIZE)
    full_keys = jnp.repeat(keys.astype(jnp.float32).reshape(WINDOW_TOKENS, KEY_VALUE_HEADS, HEAD_SIZE), QUERY_HEADS // KEY_VALUE_HEADS, axis=1)
    positions = jnp.arange(WINDOW_TOKENS, dtype=jnp.int32)

    def one_block(index):
        rows_query = query_blocks[index]
        scores = jnp.einsum('qhd,khd->hqk', rows_query, full_keys, precision=jax.lax.Precision.HIGHEST) * HEAD_SIZE ** (-0.5)
        query_pos = index * QB + jnp.arange(QB, dtype=jnp.int32)
        allowed = (documents[query_pos][:, None] == documents[None, :]) & (positions[None, :] <= query_pos[:, None])
        masked = jnp.where(allowed[None], scores, -jnp.inf)
        return jax.nn.logsumexp(masked, axis=2)
    stacked = lax.map(one_block, jnp.arange(WINDOW_TOKENS // QB, dtype=jnp.int32))
    return jnp.transpose(stacked, (1, 0, 2)).reshape(QUERY_HEADS, WINDOW_TOKENS)


def strengthened(drawn, own_key, source, target, blocks, factor):
    owner, partner = [(jnp.arange(drawn.shape[axis_at]) // (drawn.shape[axis_at] // blocks)).reshape([-1 if axis == axis_at else 1 for axis in range(drawn.ndim)]) for axis_at in (source, target)]
    chosen = jax.random.permutation(own_key, blocks)[partner]
    strong = (owner == chosen) | (owner == (partner + blocks // 2) % blocks)
    return jnp.where(strong, factor * drawn, drawn)


def level_of(key, dims, shards, least, high):
    def one(dim, parts):
        heights = jax.random.uniform(jax.random.fold_in(jax.random.fold_in(key, 6), dim), (parts,), jnp.float32, least / len(shards), high / len(shards))
        return jnp.repeat(jnp.exp(heights), dims[dim] // parts).reshape((-1,) + (1,) * (len(dims) - dim - 1))

    loudness = one(*shards[0])
    for cut in shards[1:]:
        loudness = loudness * one(*cut)
    return loudness


def gaussian(rng, dims, width, bound, cuts=(), kind=jnp.bfloat16):
    loudness = level_of(rng, dims, cuts, -0.22, 0.18) if cuts else 1.0
    values = jax.random.normal(rng, dims, jnp.float32) * width * loudness
    return jnp.minimum(jnp.maximum(values, -bound), bound).astype(kind)


def bell_draw_with(rng, extent, scale, most, cuts, heavy, kind=jnp.bfloat16):
    array = scale * jax.random.normal(rng, extent, jnp.float32)
    if cuts:
        array = array * level_of(rng, extent, cuts, -0.22, 0.18)
    return jnp.clip(strengthened(array, jax.random.fold_in(rng, 3), *heavy), -most, most).astype(kind)


def setup_inputs(seed: int = 0) -> dict:
    streams_of = jax.random.split(jax.random.key(seed), 12)
    return {
        "normed": gaussian(streams_of[0], (WINDOW_TOKENS, D), 0.05, 0.29882812, ((0, 8), (1, 32))),
        "queries": draw_queries(jax.random.fold_in(streams_of[11], 71), 0),
        "keys": draw_keys(jax.random.fold_in(streams_of[11], 71), 0),
        "values": gaussian(streams_of[3], (WINDOW_TOKENS, KEY_VALUE_HEADS * HEAD_SIZE), 1.0, 6.0, ((0, 8),)),
        "attn_out": gaussian(streams_of[4], (WINDOW_TOKENS, QUERY_HEADS * HEAD_SIZE), 0.05, 0.29882812, ((0, 8), (1, 16))),
        "row_logsumexp": draw_row_logsumexp(jax.random.fold_in(streams_of[11], 71), 0),
        "out_grad": bell_draw_with(streams_of[6], (WINDOW_TOKENS, D), 1.0, 6.0, ((0, 8), (1, 32)), (0, 1, 32, 2.75)),
        "out_weight": gaussian(streams_of[7], (QUERY_HEADS * HEAD_SIZE, D), (QUERY_HEADS * HEAD_SIZE) ** -0.5, 0.09375, ((0, 16),)),
        "qkv_weight": gaussian(streams_of[8], (D, QKV), D ** -0.5, 0.09375, ((0, 32),)),
        "documents": draw_documents(jax.random.fold_in(streams_of[11], 71), 0),
        "tasks": draw_tasks(jax.random.fold_in(streams_of[11], 71), 0),
    }


def tile_grads(block_q, block_k, queries4, grads4, keys_three, values_three, lse3, delta3, documents):
    offsets = jnp.arange(QB, dtype=jnp.int32)
    query_pos = block_q * QB + offsets
    key_pos = block_k * QB + offsets
    query_rows = lax.dynamic_slice_in_dim(queries4, block_q * QB, QB, 0)
    grad_rows = lax.dynamic_slice_in_dim(grads4, block_q * QB, QB, 0)
    key_rows = lax.dynamic_slice_in_dim(keys_three, block_k * QB, QB, 0)
    value_rows = lax.dynamic_slice_in_dim(values_three, block_k * QB, QB, 0)
    lse_rows = lax.dynamic_slice_in_dim(lse3, block_q * QB, QB, 2)
    delta_rows = lax.dynamic_slice_in_dim(delta3, block_q * QB, QB, 2)
    query_docs = lax.dynamic_slice_in_dim(documents, block_q * QB, QB, 0)
    key_docs = lax.dynamic_slice_in_dim(documents, block_k * QB, QB, 0)
    allowed = (query_docs[:, None] == key_docs[None, :]) & (key_pos[None, :] <= query_pos[:, None])
    scores = jnp.einsum('qphd,cpd->phqc', query_rows, key_rows) * HEAD_SIZE ** -0.5
    probs = jnp.exp(jnp.where(allowed, scores - lse_rows[..., None], -jnp.inf))
    probs_low = lax.optimization_barrier(probs.astype(jnp.bfloat16)).astype(jnp.float32)
    value_grad = jnp.einsum('phqc,qphd->cpd', probs_low, grad_rows)
    prob_grad = jnp.einsum('qphd,cpd->phqc', grad_rows, value_rows)
    score_grad = (probs * (prob_grad - delta_rows[..., None]) * HEAD_SIZE ** -0.5).astype(jnp.bfloat16)
    score_grad = lax.optimization_barrier(score_grad).astype(jnp.float32)
    query_grad = jnp.einsum('phqc,cpd->qphd', score_grad, key_rows)
    key_grad = jnp.einsum('phqc,qphd->cpd', score_grad, query_rows)
    return query_grad, jnp.stack([key_grad, value_grad], axis=2)


def block_sums(left, right):
    left3 = left.reshape(SERVERS, -1, left.shape[1])
    right3 = right.reshape(SERVERS, -1, right.shape[1])

    def accumulate(running, pieces):
        partial_value = jnp.dot(pieces[0].T, pieces[1], preferred_element_type=jnp.float32)
        return running + lax.optimization_barrier(partial_value.astype(jnp.bfloat16)).astype(jnp.float32), None

    summed, ignored = lax.scan(accumulate, jnp.zeros((left.shape[1], right.shape[1]), jnp.float32), (left3, right3))
    return summed.astype(jnp.bfloat16)


def reference(normed, queries, keys, values, attn_out, row_logsumexp, out_grad, out_weight, qkv_weight, documents, tasks):
    grand_total = normed.shape[0]
    block_count = grand_total // QB
    pair_count = QUERY_HEADS // 2
    attn_grad = jnp.dot(out_grad, out_weight.T, preferred_element_type=jnp.float32).astype(jnp.bfloat16)
    grads4 = attn_grad.astype(jnp.float32).reshape(grand_total, pair_count, 2, HEAD_SIZE)
    queries4 = queries.astype(jnp.float32).reshape(grand_total, pair_count, 2, HEAD_SIZE)
    outputs4 = attn_out.astype(jnp.float32).reshape(grand_total, pair_count, 2, HEAD_SIZE)
    delta3 = jnp.transpose(jnp.sum(grads4 * outputs4, axis=3), (1, 2, 0))
    keys_three = jnp.repeat(keys.astype(jnp.float32).reshape(grand_total, KEY_VALUE_HEADS, HEAD_SIZE), 2, axis=1)
    values_three = jnp.repeat(values.astype(jnp.float32).reshape(grand_total, KEY_VALUE_HEADS, HEAD_SIZE), 2, axis=1)
    lse3 = row_logsumexp.reshape(pair_count, 2, grand_total)
    slot_blocks = tasks[:, :, 0].reshape(-1)
    slot_firsts = tasks[:, :, 1].reshape(-1)
    matches = (slot_blocks[None, :] == jnp.arange(block_count, dtype=jnp.int32)[:, None]).astype(jnp.int32)
    first_blocks = jnp.sum(matches * slot_firsts[None, :], axis=1).astype(jnp.int32)

    def query_block(block_q, carry):
        query_all, pair_all = carry

        def key_block(block_k, inner):
            partial_q, pairs_acc = inner
            tile_q, tile_kv = tile_grads(block_q, block_k, queries4, grads4, keys_three, values_three, lse3, delta3, documents)
            current = lax.dynamic_slice_in_dim(pairs_acc, block_k * QB, QB, 0)
            pairs_acc = lax.dynamic_update_slice_in_dim(pairs_acc, current + tile_kv, block_k * QB, 0)
            return partial_q + tile_q, pairs_acc

        start = jnp.zeros((QB, pair_count, 2, HEAD_SIZE), jnp.float32)
        partial_q, pair_all = lax.fori_loop(first_blocks[block_q], block_q + 1, key_block, (start, pair_all))
        rounded = partial_q.reshape(QB, QUERY_HEADS * HEAD_SIZE).astype(jnp.bfloat16)
        query_all = lax.dynamic_update_slice_in_dim(query_all, rounded, block_q * QB, 0)
        return query_all, pair_all

    initial = (jnp.zeros((grand_total, QUERY_HEADS * HEAD_SIZE), jnp.bfloat16), jnp.zeros((grand_total, pair_count, 2, HEAD_SIZE), jnp.float32))
    query_grads, pair_sums = lax.fori_loop(jnp.int32(0), jnp.int32(block_count), query_block, initial)
    lower_pair = lax.optimization_barrier(pair_sums.astype(jnp.bfloat16)).astype(jnp.float32)
    grouped_queries = jnp.sum(lower_pair.reshape(grand_total, KEY_VALUE_HEADS, 2, 2, HEAD_SIZE), axis=2).astype(jnp.bfloat16)
    key_gradients = grouped_queries[:, :, 0, :].reshape(grand_total, KEY_VALUE_HEADS * HEAD_SIZE)
    value_gradients = grouped_queries[:, :, 1, :].reshape(grand_total, KEY_VALUE_HEADS * HEAD_SIZE)
    qkv_grads = jnp.concatenate([query_grads, key_gradients, value_gradients], axis=1)
    normed_grad = jnp.dot(qkv_grads, qkv_weight.T, preferred_element_type=jnp.float32).astype(jnp.bfloat16)
    return normed_grad, block_sums(attn_out, out_grad), block_sums(normed, qkv_grads)
```

```python
import jax
import jax.numpy as jnp
from jax import lax
from jax.experimental import pallas as pl
from jax.experimental.pallas import tpu as pltpu
from jax.sharding import PartitionSpec as P

MESH = pl.DeviceIdType.MESH
D = 4096
QUERY_HEADS = 32
KEY_VALUE_HEADS = 8
HEAD_SIZE = 128
QB = 256
BLOCKS = 16
LOG2E = 1.4426950408889634
SCALE = HEAD_SIZE ** (-0.5)
NT = (((1,), (1,)), ((), ()))
TN = (((0,), (0,)), ((), ()))
NN = (((1,), (0,)), ((), ()))


def dot(a, b, dims):
    return lax.dot_general(a, b, dims, preferred_element_type=jnp.float32)


def remote(src, dst, send, recv, where):
    return pltpu.make_async_remote_copy(
        src_ref=src, dst_ref=dst, send_sem=send, recv_sem=recv, device_id=where, device_id_type=MESH
    )


def greet(places):
    barrier = pltpu.get_barrier_semaphore()
    for where in places:
        pl.semaphore_signal(barrier, inc=1, device_id=where, device_id_type=MESH)
    pl.semaphore_wait(barrier, len(places))


def place():
    r = lax.axis_index("role")
    w = lax.axis_index("wide")
    t = lax.axis_index("tp")
    return r, w, t, t // 2, t % 2


def plane_peer(w, z, xl, k):
    dx, dy = k // 4, k % 4
    peer = ((w // 4 + dx) % 2) * 4 + (w % 4 + dy) % 4
    return {"wide": peer, "tp": z * 2 + (xl if dx == 0 else 1 - xl)}


def front_kernel(
    og, ow, keys, values, ao, ag_out, kv, part, G, O, W, A, acc,
    lsem, swap_sem, x_sem, z_send, z_recv, k_send, k_recv, kp_sem, p_send, p_recv,
):
    r, w, t, z, xl = place()
    partner = {"role": 1 - r}
    inner = {"tp": z * 2 + 1 - xl}
    up = {"tp": ((z + 1) % 8) * 2 + xl}
    down = {"tp": ((z + 7) % 8) * 2 + xl}
    cols = pl.ds(pl.multiple_of(xl * 128, 128), 128)
    mine = pl.ds(pl.multiple_of(r * QB, QB), QB)
    other = pl.ds(pl.multiple_of((1 - r) * QB, QB), QB)
    heads = pl.ds(pl.multiple_of(z * 128, 128), 128)

    @pl.when(r == 0)
    def _():
        pltpu.make_async_copy(keys.at[:, heads], kv.at[r, w], lsem.at[0]).start()

    @pl.when(r == 1)
    def _():
        pltpu.make_async_copy(values.at[:, heads], kv.at[r, w], lsem.at[0]).start()

    load_own = pltpu.make_async_copy(og.at[mine, :], G.at[z, r, :, cols], lsem.at[1])
    load_own.start()
    load_w = pltpu.make_async_copy(ow, W, lsem.at[2])
    load_w.start()
    load_a = pltpu.make_async_copy(ao, A, lsem.at[3])
    load_a.start()

    peers = [plane_peer(w, z, xl, k) for k in range(1, 8)]
    greet([partner, inner, up, down] + peers)

    swap = remote(
        og.at[other, :], G.at[z, r, :, cols], swap_sem.at[0], swap_sem.at[1], partner
    )
    swap.start()
    pltpu.make_async_copy(keys.at[:, heads], kv.at[r, w], lsem.at[0]).wait()
    pushes = []
    for k in range(7):
        c = remote(kv.at[r, w], kv.at[r, w], k_send.at[k], k_recv.at[k], peers[k])
        c.start()
        pushes.append(c)
    load_own.wait()
    swap.wait_recv()
    cross = remote(
        G.at[z, :, :, cols], G.at[z, :, :, cols], x_sem.at[0], x_sem.at[1], inner
    )
    cross.start()
    load_w.wait()
    load_a.wait()
    acc[...] = jnp.zeros_like(acc)
    cross.wait_recv()

    sends = [swap, cross]
    order = []
    hands = []

    def ring(s):
        pair = []
        for d, where in ((0, up), (1, down)):
            at = (z + 8 - s) % 8 if d == 0 else (z + s) % 8
            ref = G.at[at] if s < 3 else G.at[at, d]
            c = remote(ref, ref, z_send.at[d, s], z_recv.at[d, s], where)
            c.start()
            pair.append(c)
            sends.append(c)
        return pair

    def use(at):
        k = len(order)
        hand = remote(G.at[at, 1 - r], O.at[at], p_send.at[k], p_recv.at[k], partner)
        hand.start()
        order.append(at)
        hands.append(hand)
        low = pl.ds(pl.multiple_of(at * QB, QB), QB)
        high = pl.ds(pl.multiple_of(2048 + at * QB, QB), QB)
        acc[...] += dot(G[at, 0], W[:, low], NT) + dot(G[at, 1], W[:, high], NT)

    def product(k):
        at = order[k]
        hands[k].wait_recv()
        total = dot(A[mine, :], G[at, r], TN) + dot(A[other, :], O[at], TN)
        part[at] = total.astype(part.dtype)

    pair = ring(0)
    use(z)
    for s in range(1, 4):
        pair[0].wait_recv()
        pair[1].wait_recv()
        pair = ring(s)
        use((z + 8 - s) % 8)
        use((z + s) % 8)
        if s == 2:
            product(0)
        if s == 3:
            for c in pushes:
                c.wait_recv()
            hand_kv = remote(kv.at[r], kv.at[r], kp_sem.at[0], kp_sem.at[1], partner)
            hand_kv.start()
            for k in (1, 2, 3, 4):
                product(k)
    pair[0].wait_recv()
    pair[1].wait_recv()
    use((z + 4) % 8)
    ag_out[...] = acc[...].astype(ag_out.dtype)
    for k in (5, 6, 7):
        product(k)
    hand_kv.wait_recv()
    hand_kv.wait_send()
    for c in sends + pushes + hands:
        c.wait_send()


def front(out_grad, out_weight, keys, values, attn_out):
    hbm = pl.BlockSpec(memory_space=pltpu.HBM)
    vmem = pl.BlockSpec(memory_space=pltpu.VMEM)
    dma = pltpu.SemaphoreType.DMA
    return pl.pallas_call(
        front_kernel,
        name="front",
        out_shape=(
            jax.ShapeDtypeStruct((QB, QB), jnp.bfloat16),
            jax.ShapeDtypeStruct((2, 8, 512, 128), jnp.bfloat16),
            jax.ShapeDtypeStruct((8, QB, QB), jnp.bfloat16),
        ),
        in_specs=[hbm] * 5,
        out_specs=(vmem, vmem, vmem),
        scratch_shapes=[
            pltpu.VMEM((8, 2, QB, QB), jnp.bfloat16),
            pltpu.VMEM((8, QB, QB), jnp.bfloat16),
            pltpu.VMEM((QB, D), jnp.bfloat16),
            pltpu.VMEM((512, QB), jnp.bfloat16),
            pltpu.VMEM((QB, QB), jnp.float32),
            dma((4,)), dma((2,)), dma((2,)), dma((2, 4)), dma((2, 4)),
            dma((7,)), dma((7,)), dma((2,)), dma((8,)), dma((8,)),
        ],
        compiler_params=pltpu.CompilerParams(
            collective_id=0, has_side_effects=True, vmem_limit_bytes=40 * 1024 * 1024
        ),
        cost_estimate=pl.CostEstimate(flops=2_000_000_000, bytes_accessed=20_000_000, transcendentals=0),
    )(out_grad, out_weight, keys, values, attn_out)


def first_at_least(docs, value):
    def step(_, span):
        low, high = span
        mid = (low + high) // 2
        below = docs[jnp.minimum(mid, 4095)] < value
        live = low < high
        return (
            jnp.where(live & below, mid + 1, low),
            jnp.where(live & jnp.logical_not(below), mid, high),
        )

    return lax.fori_loop(0, 13, step, (jnp.int32(0), jnp.int32(4096)))[0]


def attn_kernel(docs, q_ref, ag, ao, lse, kv, dq_out, dkv, q2, g2, dq):
    r, w, t, z, xl = place()
    block = 2 * w + r
    start_at = block * QB
    rows = pl.ds(pl.multiple_of(r * QB, QB), QB)
    second = first_at_least(docs, 1)
    third = first_at_least(docs, 2)

    def doc_start(at):
        return jnp.where(at >= third, third, jnp.where(at >= second, second, 0))

    span = pl.ds(pl.multiple_of(start_at, QB), QB)
    deltas, lses = [], []
    for h in range(2):
        hc = pl.ds(h * 128, 128)
        q2[pl.ds(h * QB, QB), :] = q_ref[rows, hc]
        g = ag[:, hc]
        g2[pl.ds(h * QB, QB), :] = g
        both = g.astype(jnp.float32) * ao[rows, hc].astype(jnp.float32)
        deltas.append(jnp.sum(both.T, axis=0, keepdims=True))
        lses.append(lse[pl.ds(h, 1), span] * LOG2E)
    delta = jnp.concatenate(deltas, axis=1)
    lse2 = jnp.concatenate(lses, axis=1)
    lane = lax.broadcasted_iota(jnp.int32, (1, 2 * QB), 1)
    q_pos = start_at + jnp.where(lane >= QB, lane - QB, lane)
    q_start = doc_start(q_pos)
    dq[...] = jnp.zeros_like(dq)
    dkv[...] = jnp.zeros_like(dkv)

    @pl.loop(doc_start(start_at) // QB, block + 1)
    def _(kb):
        k_rows = kv[0, kb]
        v_rows = kv[1, kb]
        scores = dot(k_rows, q2[...], NT)
        k_pos = kb * QB + lax.broadcasted_iota(jnp.int32, (QB, 1), 0)
        allowed = (k_pos <= q_pos) & (k_pos >= q_start)
        probs = jnp.where(allowed, jnp.exp2(scores * (SCALE * LOG2E) - lse2), 0.0)
        dv = dot(probs.astype(jnp.bfloat16), g2[...], NN)
        prob_grad = dot(v_rows, g2[...], NT)
        ds = (probs * (prob_grad - delta)).astype(jnp.bfloat16)
        dk = dot(ds, q2[...], NN) * SCALE
        dq[...] += dot(ds, k_rows, TN)
        dkv[kb // 2, kb % 2, :, 0:128] = dk.astype(jnp.bfloat16)
        dkv[kb // 2, kb % 2, :, 128:256] = dv.astype(jnp.bfloat16)

    for h in range(2):
        dq_out[:, h * 128:(h + 1) * 128] = (dq[pl.ds(h * QB, QB), :] * SCALE).astype(jnp.bfloat16)


def attend(documents, queries, attn_grad, attn_out, lse, kv):
    vmem = pl.BlockSpec(memory_space=pltpu.VMEM)
    return pl.pallas_call(
        attn_kernel,
        name="attend",
        out_shape=(
            jax.ShapeDtypeStruct((QB, QB), jnp.bfloat16),
            jax.ShapeDtypeStruct((8, 2, QB, QB), jnp.bfloat16),
        ),
        in_specs=[pl.BlockSpec(memory_space=pltpu.SMEM)] + [vmem] * 5,
        out_specs=(vmem, vmem),
        scratch_shapes=[
            pltpu.VMEM((2 * QB, 128), jnp.bfloat16),
            pltpu.VMEM((2 * QB, 128), jnp.bfloat16),
            pltpu.VMEM((2 * QB, 128), jnp.float32),
        ],
        compiler_params=pltpu.CompilerParams(vmem_limit_bytes=40 * 1024 * 1024),
        cost_estimate=pl.CostEstimate(
            flops=5_000_000_000, bytes_accessed=6_000_000, transcendentals=2_000_000
        ),
    )(documents, queries, attn_grad, attn_out, lse, kv)


def cut_along(shard, dim, length):
    before, after = (shard.shape[:dim], shard.shape[dim + 1 :])
    return jnp.moveaxis(shard.reshape(*before, length, -1, *after), dim, 0)


def sum_at_owner(shard, axis, dim):
    tiles = cut_along(shard, dim, lax.axis_size(axis))
    arrived = lax.all_to_all(tiles, axis, split_axis=0, concat_axis=0, tiled=True)
    return arrived.astype(jnp.float32).sum(axis=0)


def in_one_piece(arrays, axis, dim, along):
    both = jnp.concatenate(arrays, axis=along)
    out, at, done = (lax.all_gather(both, axis, axis=dim, tiled=True), 0, [])
    for a in arrays:
        done.append(lax.slice_in_dim(out, at, at + a.shape[along], axis=along))
        at += a.shape[along]
    return tuple(done)


def local(
    normed, queries, keys, values, attn_out, row_logsumexp, out_grad, out_weight, qkv_weight, documents, tasks
):
    row_halves = QB
    local_rows = 512
    attn_grad, kv, part = front(out_grad, out_weight, keys, values, attn_out)
    arrived = lax.all_to_all(part, "wide", split_axis=0, concat_axis=0, tiled=True)
    out_sum = arrived.astype(jnp.float32).sum(axis=0)
    query_piece, dkv = attend(
        documents, queries, attn_grad, attn_out, row_logsumexp, kv.reshape(2, BLOCKS, QB, 128)
    )
    kv_flat = dkv.transpose(1, 0, 2, 3).reshape(BLOCKS * QB, QB)
    kv_sum = sum_at_owner(kv_flat, ("role", "wide"), 0)
    head_q, key_value_head = in_one_piece(
        (query_piece, kv_sum.astype(jnp.bfloat16)), ("role", "tp"), 1, 0
    )
    query_grads = head_q.reshape(row_halves, 2, QUERY_HEADS * HEAD_SIZE)
    grouped_queries = jnp.sum(
        key_value_head.reshape(row_halves, 2, KEY_VALUE_HEADS, 2, 2 * HEAD_SIZE).astype(
            jnp.float32
        ),
        axis=3,
    ).astype(jnp.bfloat16)
    key_gradients = grouped_queries[..., :HEAD_SIZE].reshape(
        row_halves, 2, KEY_VALUE_HEADS * HEAD_SIZE
    )
    value_gradients = grouped_queries[..., HEAD_SIZE:].reshape(
        row_halves, 2, KEY_VALUE_HEADS * HEAD_SIZE
    )
    qkv_grads = jnp.concatenate([query_grads, key_gradients, value_gradients], axis=2)
    normed_grad = jnp.einsum(
        "irc,nc->rin", qkv_grads, qkv_weight, preferred_element_type=jnp.float32
    )
    normed_grad = normed_grad.reshape(local_rows, qkv_weight.shape[0]).astype(jnp.bfloat16)
    qkv_part = jnp.einsum(
        "rin,irc->nc",
        normed.reshape(2, row_halves, normed.shape[1]),
        qkv_grads,
        preferred_element_type=jnp.float32,
    )
    qkv_sum = sum_at_owner(qkv_part.astype(jnp.bfloat16), "wide", 1)
    return (normed_grad, out_sum.astype(jnp.bfloat16), qkv_sum.astype(jnp.bfloat16))


def solution(mesh):
    in_specs = (
        P("wide", ("role", "tp")),
        P("wide", "tp"),
        P("wide", None),
        P("wide", None),
        P("wide", "tp"),
        P("tp", None),
        P("wide", ("role", "tp")),
        P("tp", None),
        P(("role", "tp"), None),
        P(),
        P(),
    )
    out_specs = (P("wide", ("role", "tp")), P("tp", ("role", "wide")), P(("role", "tp"), "wide"))
    return jax.shard_map(local, mesh=mesh, in_specs=in_specs, out_specs=out_specs, check_vma=False)
```

```python
import jax
import jax.numpy as jnp
from jax import lax
from jax.experimental import pallas as pl
from jax.experimental.pallas import tpu as pltpu
from jax.sharding import PartitionSpec as P

MESH = pl.DeviceIdType.MESH
D = 4096
QUERY_HEADS = 32
KEY_VALUE_HEADS = 8
HEAD_SIZE = 128
QB = 256
BLOCKS = 16
LOG2E = 1.4426950408889634
SCALE = HEAD_SIZE ** (-0.5)
NT = (((1,), (1,)), ((), ()))
TN = (((0,), (0,)), ((), ()))
NN = (((1,), (0,)), ((), ()))


def dot(a, b, dims):
    return lax.dot_general(a, b, dims, preferred_element_type=jnp.float32)


def remote(src, dst, send, recv, where):
    return pltpu.make_async_remote_copy(
        src_ref=src, dst_ref=dst, send_sem=send, recv_sem=recv, device_id=where, device_id_type=MESH
    )


def greet(places):
    barrier = pltpu.get_barrier_semaphore()
    for where in places:
        pl.semaphore_signal(barrier, inc=1, device_id=where, device_id_type=MESH)
    pl.semaphore_wait(barrier, len(places))


def place():
    r = lax.axis_index("role")
    w = lax.axis_index("wide")
    t = lax.axis_index("tp")
    return r, w, t, t // 2, t % 2


def plane_peer(w, z, xl, k):
    dx, dy = k // 4, k % 4
    peer = ((w // 4 + dx) % 2) * 4 + (w % 4 + dy) % 4
    return {"wide": peer, "tp": z * 2 + (xl if dx == 0 else 1 - xl)}


def front_kernel(
    og, ow, keys, values, ao, ag_out, kv, part, G, O, W, A, acc,
    lsem, swap_sem, x_sem, z_send, z_recv, k_send, k_recv, kp_sem, p_send, p_recv,
):
    r, w, t, z, xl = place()
    partner = {"role": 1 - r}
    inner = {"tp": z * 2 + 1 - xl}
    up = {"tp": ((z + 1) % 8) * 2 + xl}
    down = {"tp": ((z + 7) % 8) * 2 + xl}
    cols = pl.ds(pl.multiple_of(xl * 128, 128), 128)
    mine = pl.ds(pl.multiple_of(r * QB, QB), QB)
    other = pl.ds(pl.multiple_of((1 - r) * QB, QB), QB)
    heads = pl.ds(pl.multiple_of(z * 128, 128), 128)

    @pl.when(r == 0)
    def _():
        pltpu.make_async_copy(keys.at[:, heads], kv.at[r, w], lsem.at[0]).start()

    @pl.when(r == 1)
    def _():
        pltpu.make_async_copy(values.at[:, heads], kv.at[r, w], lsem.at[0]).start()

    load_own = pltpu.make_async_copy(og.at[mine, :], G.at[z, r, :, cols], lsem.at[1])
    load_own.start()
    load_w = pltpu.make_async_copy(ow, W, lsem.at[2])
    load_w.start()
    load_a = pltpu.make_async_copy(ao, A, lsem.at[3])
    load_a.start()

    peers = [plane_peer(w, z, xl, k) for k in range(1, 8)]
    greet([partner, inner, up, down] + peers)

    swap = remote(
        og.at[other, :], G.at[z, r, :, cols], swap_sem.at[0], swap_sem.at[1], partner
    )
    swap.start()
    pltpu.make_async_copy(keys.at[:, heads], kv.at[r, w], lsem.at[0]).wait()
    pushes = []
    for k in range(7):
        c = remote(kv.at[r, w], kv.at[r, w], k_send.at[k], k_recv.at[k], peers[k])
        c.start()
        pushes.append(c)
    load_own.wait()
    swap.wait_recv()
    cross = remote(
        G.at[z, :, :, cols], G.at[z, :, :, cols], x_sem.at[0], x_sem.at[1], inner
    )
    cross.start()
    load_w.wait()
    load_a.wait()
    acc[...] = jnp.zeros_like(acc)
    cross.wait_recv()

    sends = [swap, cross]
    order = []
    hands = []

    def ring(s):
        pair = []
        for d, where in ((0, up), (1, down)):
            at = (z + 8 - s) % 8 if d == 0 else (z + s) % 8
            ref = G.at[at] if s < 3 else G.at[at, d]
            c = remote(ref, ref, z_send.at[d, s], z_recv.at[d, s], where)
            c.start()
            pair.append(c)
            sends.append(c)
        return pair

    def use(at):
        k = len(order)
        hand = remote(G.at[at, 1 - r], O.at[at], p_send.at[k], p_recv.at[k], partner)
        hand.start()
        order.append(at)
        hands.append(hand)
        low = pl.ds(pl.multiple_of(at * QB, QB), QB)
        high = pl.ds(pl.multiple_of(2048 + at * QB, QB), QB)
        acc[...] += dot(G[at, 0], W[:, low], NT) + dot(G[at, 1], W[:, high], NT)

    def product(k):
        at = order[k]
        hands[k].wait_recv()
        total = dot(A[mine, :], G[at, r], TN) + dot(A[other, :], O[at], TN)
        part[at] = total.astype(part.dtype)

    pair = ring(0)
    use(z)
    for s in range(1, 4):
        pair[0].wait_recv()
        pair[1].wait_recv()
        pair = ring(s)
        use((z + 8 - s) % 8)
        use((z + s) % 8)
        if s == 2:
            product(0)
        if s == 3:
            for c in pushes:
                c.wait_recv()
            hand_kv = remote(kv.at[r], kv.at[r], kp_sem.at[0], kp_sem.at[1], partner)
            hand_kv.start()
            for k in (1, 2, 3, 4):
                product(k)
    pair[0].wait_recv()
    pair[1].wait_recv()
    use((z + 4) % 8)
    ag_out[...] = acc[...].astype(ag_out.dtype)
    for k in (5, 6, 7):
        product(k)
    hand_kv.wait_recv()
    hand_kv.wait_send()
    for c in sends + pushes + hands:
        c.wait_send()


def front(out_grad, out_weight, keys, values, attn_out):
    hbm = pl.BlockSpec(memory_space=pltpu.HBM)
    vmem = pl.BlockSpec(memory_space=pltpu.VMEM)
    dma = pltpu.SemaphoreType.DMA
    return pl.pallas_call(
        front_kernel,
        name="front",
        out_shape=(
            jax.ShapeDtypeStruct((QB, QB), jnp.bfloat16),
            jax.ShapeDtypeStruct((2, 8, 512, 128), jnp.bfloat16),
            jax.ShapeDtypeStruct((8, QB, QB), jnp.bfloat16),
        ),
        in_specs=[hbm] * 5,
        out_specs=(vmem, vmem, vmem),
        scratch_shapes=[
            pltpu.VMEM((8, 2, QB, QB), jnp.bfloat16),
            pltpu.VMEM((8, QB, QB), jnp.bfloat16),
            pltpu.VMEM((QB, D), jnp.bfloat16),
            pltpu.VMEM((512, QB), jnp.bfloat16),
            pltpu.VMEM((QB, QB), jnp.float32),
            dma((4,)), dma((2,)), dma((2,)), dma((2, 4)), dma((2, 4)),
            dma((7,)), dma((7,)), dma((2,)), dma((8,)), dma((8,)),
        ],
        compiler_params=pltpu.CompilerParams(
            collective_id=0, has_side_effects=True, vmem_limit_bytes=40 * 1024 * 1024
        ),
        cost_estimate=pl.CostEstimate(flops=2_000_000_000, bytes_accessed=20_000_000, transcendentals=0),
    )(out_grad, out_weight, keys, values, attn_out)


def first_at_least(docs, value):
    def step(_, span):
        low, high = span
        mid = (low + high) // 2
        below = docs[jnp.minimum(mid, 4095)] < value
        live = low < high
        return (
            jnp.where(live & below, mid + 1, low),
            jnp.where(live & jnp.logical_not(below), mid, high),
        )

    return lax.fori_loop(0, 13, step, (jnp.int32(0), jnp.int32(4096)))[0]


def attn_kernel(docs, q_ref, ag, ao, lse, kv, dq_out, dkv, q2, g2, dq):
    r, w, t, z, xl = place()
    block = 2 * w + r
    start_at = block * QB
    rows = pl.ds(pl.multiple_of(r * QB, QB), QB)
    second = first_at_least(docs, 1)
    third = first_at_least(docs, 2)

    def doc_start(at):
        return jnp.where(at >= third, third, jnp.where(at >= second, second, 0))

    span = pl.ds(pl.multiple_of(start_at, QB), QB)
    deltas, lses = [], []
    for h in range(2):
        hc = pl.ds(h * 128, 128)
        q2[pl.ds(h * QB, QB), :] = q_ref[rows, hc]
        g = ag[:, hc]
        g2[pl.ds(h * QB, QB), :] = g
        both = g.astype(jnp.float32) * ao[rows, hc].astype(jnp.float32)
        deltas.append(jnp.sum(both.T, axis=0, keepdims=True))
        lses.append(lse[pl.ds(h, 1), span] * LOG2E)
    delta = jnp.concatenate(deltas, axis=1)
    lse2 = jnp.concatenate(lses, axis=1)
    lane = lax.broadcasted_iota(jnp.int32, (1, 2 * QB), 1)
    q_pos = start_at + jnp.where(lane >= QB, lane - QB, lane)
    q_start = doc_start(q_pos)
    dq[...] = jnp.zeros_like(dq)
    dkv[...] = jnp.zeros_like(dkv)

    @pl.loop(doc_start(start_at) // QB, block + 1)
    def _(kb):
        k_rows = kv[0, kb]
        v_rows = kv[1, kb]
        scores = dot(k_rows, q2[...], NT)
        k_pos = kb * QB + lax.broadcasted_iota(jnp.int32, (QB, 1), 0)
        allowed = (k_pos <= q_pos) & (k_pos >= q_start)
        probs = jnp.where(allowed, jnp.exp2(scores * (SCALE * LOG2E) - lse2), 0.0)
        dv = dot(probs.astype(jnp.bfloat16), g2[...], NN)
        prob_grad = dot(v_rows, g2[...], NT)
        ds = (probs * (prob_grad - delta)).astype(jnp.bfloat16)
        dk = dot(ds, q2[...], NN) * SCALE
        dq[...] += dot(ds, k_rows, TN)
        dkv[kb // 2, kb % 2, :, 0:128] = dk.astype(jnp.bfloat16)
        dkv[kb // 2, kb % 2, :, 128:256] = dv.astype(jnp.bfloat16)

    for h in range(2):
        dq_out[:, h * 128:(h + 1) * 128] = (dq[pl.ds(h * QB, QB), :] * SCALE).astype(jnp.bfloat16)


def attend(documents, queries, attn_grad, attn_out, lse, kv):
    vmem = pl.BlockSpec(memory_space=pltpu.VMEM)
    return pl.pallas_call(
        attn_kernel,
        name="attend",
        out_shape=(
            jax.ShapeDtypeStruct((QB, QB), jnp.bfloat16),
            jax.ShapeDtypeStruct((8, 2, QB, QB), jnp.bfloat16),
        ),
        in_specs=[pl.BlockSpec(memory_space=pltpu.SMEM)] + [vmem] * 5,
        out_specs=(vmem, vmem),
        scratch_shapes=[
            pltpu.VMEM((2 * QB, 128), jnp.bfloat16),
            pltpu.VMEM((2 * QB, 128), jnp.bfloat16),
            pltpu.VMEM((2 * QB, 128), jnp.float32),
        ],
        compiler_params=pltpu.CompilerParams(vmem_limit_bytes=40 * 1024 * 1024),
        cost_estimate=pl.CostEstimate(
            flops=5_000_000_000, bytes_accessed=6_000_000, transcendentals=2_000_000
        ),
    )(documents, queries, attn_grad, attn_out, lse, kv)


def back_kernel(
    dq, dkv, normed, wq, ng_out, gw_out, QF, KF, D1, S, D2, F, FR, N, nacc, kacc,
    lsem, d1s, d1r, d2s, d2r, x_sem, z_send, z_recv, p_send, p_recv, kx_sem, kz_send, kz_recv,
    kp_send, kp_recv, f_send, f_recv,
):
    r, w, t, z, xl = place()
    partner = {"role": 1 - r}
    inner = {"tp": z * 2 + 1 - xl}
    up = {"tp": ((z + 1) % 8) * 2 + xl}
    down = {"tp": ((z + 7) % 8) * 2 + xl}
    plane = [{"wide": (w + k // 2) % 8, "tp": z * 2 + (xl + k % 2) % 2} for k in range(1, 16)]
    load_n = pltpu.make_async_copy(normed, N, lsem.at[0])
    load_n.start()
    keep = pltpu.make_async_copy(dq, QF.at[r, z, xl], lsem.at[1])
    keep.start()
    greet([partner, up, down] + plane)

    def first(wp):
        return remote(dkv.at[wp, 1 - r], D1.at[wp], d1s.at[wp], d1r.at[wp], partner)

    @pl.loop(0, w + 1)
    def _(i):
        first(w - i).start()

    cross = remote(dq, QF.at[r, z, xl], x_sem.at[0], x_sem.at[1], inner)
    cross.start()

    def second(wp, kind):
        return remote(
            S.at[wp, kind], D2.at[w, xl], d2s.at[wp, kind], d2r.at[w, xl],
            {"wide": wp, "tp": z * 2 + kind},
        )

    def arrive(ws, xs):
        return remote(
            S.at[w, xl], D2.at[ws, xs], d2s.at[w, xl], d2r.at[ws, xs],
            {"wide": ws, "tp": z * 2 + xs},
        )

    def pair_sum(wp):
        first(wp).wait_recv()
        both = dkv[wp, r].astype(jnp.float32) + D1[wp].astype(jnp.float32)
        low = both.astype(jnp.bfloat16)
        S[wp, 0] = low[:, 0:128]
        S[wp, 1] = low[:, 128:256]

    pair_sum(w)
    second(w, 1 - xl).start()

    @pl.loop(0, w)
    def _(i):
        wp = w - 1 - i
        pair_sum(wp)
        second(wp, 0).start()
        second(wp, 1).start()

    keep.wait()
    cross.wait_recv()
    load_n.wait()
    nacc[...] = jnp.zeros_like(nacc)
    sends = [cross]
    order, hands, k_order, k_hands = [], [], [], []

    def ring(buf, ss, rs, s):
        pair = []
        for d, where in ((0, up), (1, down)):
            at = (z + 8 - s) % 8 if d == 0 else (z + s) % 8
            ref = buf.at[r, at] if s < 3 else buf.at[r, at, d]
            c = remote(ref, ref, ss.at[d, s], rs.at[d, s], where)
            c.start()
            pair.append(c)
            sends.append(c)
        return pair

    def hand(buf, ss, rs, at, seen, copies):
        c = remote(buf.at[r, at], buf.at[r, at], ss.at[len(seen)], rs.at[len(seen)], partner)
        c.start()
        seen.append(at)
        copies.append(c)

    def handed(buf, ss, rs, k, seen):
        remote(buf.at[1 - r, seen[k]], buf.at[1 - r, seen[k]], ss.at[k], rs.at[k], partner).wait_recv()

    def process(k):
        handed(QF, p_send, p_recv, k, order)
        at = order[k]
        for x in range(2):
            cols = pl.ds(pl.multiple_of((2 * at + x) * QB, QB), QB)
            weight = wq[:, cols]
            for h in range(2):
                nacc[h] += dot(QF[h, at, x], weight, NT)
            total = dot(N[0:QB, :], QF[0, at, x], TN) + dot(N[QB:512, :], QF[1, at, x], TN)
            low = total.astype(jnp.bfloat16)
            F[4 * at + 2 * x] = low[:, 0:128]
            F[4 * at + 2 * x + 1] = low[:, 128:256]

    def process_kv(k):
        handed(KF, kp_send, kp_recv, k, k_order)
        at = k_order[k]
        for x in range(2):
            cols = pl.ds(pl.multiple_of(4096 + x * 1024 + at * 128, 128), 128)
            weight = wq[:, cols]
            for h in range(2):
                nacc[h] += dot(KF[h, at, x], weight, NT)
            total = dot(N[0:QB, :], KF[0, at, x], TN) + dot(N[QB:512, :], KF[1, at, x], TN)
            F[32 + 8 * x + at] = total.astype(jnp.bfloat16)

    def chunk(wp):
        return remote(
            F.at[pl.ds(6 * wp, 6)], FR.at[w], f_send.at[wp], f_recv.at[w], {"wide": wp}
        )

    def chunk_in(ws):
        return remote(F.at[pl.ds(6 * w, 6)], FR.at[ws], f_send.at[w], f_recv.at[ws], {"wide": ws})

    def away(a):
        d = (a + 8 - z) % 8
        return jnp.minimum(d, 8 - d)

    def ship(s):
        @pl.loop(0, 5)
        def _(wp):
            ready = jnp.maximum(away((3 * wp) // 2), away((3 * wp + 2) // 2))

            @pl.when((ready == s) & (wp != w))
            def _():
                chunk(wp).start()

    pair = ring(QF, z_send, z_recv, 0)
    hand(QF, p_send, p_recv, z, order, hands)

    pair[0].wait_recv()
    pair[1].wait_recv()
    pair = ring(QF, z_send, z_recv, 1)
    hand(QF, p_send, p_recv, (z + 7) % 8, order, hands)
    hand(QF, p_send, p_recv, (z + 1) % 8, order, hands)
    process(0)

    arrive(w, 1 - xl).wait_recv()
    kacc[...] = S[w, xl].astype(jnp.float32) + D2[w, 1 - xl].astype(jnp.float32)

    @pl.loop(w + 1, 8)
    def _(ws):
        for xs in range(2):
            arrive(ws, xs).wait_recv()
            kacc[...] += D2[ws, xs].astype(jnp.float32)

    KF[r, z, xl] = kacc[...].astype(jnp.bfloat16)
    kcross = remote(KF.at[r, z, xl], KF.at[r, z, xl], kx_sem.at[0], kx_sem.at[1], inner)
    kcross.start()
    sends.append(kcross)
    process(1)
    process(2)
    ship(1)

    pair[0].wait_recv()
    pair[1].wait_recv()
    pair = ring(QF, z_send, z_recv, 2)
    hand(QF, p_send, p_recv, (z + 6) % 8, order, hands)
    hand(QF, p_send, p_recv, (z + 2) % 8, order, hands)
    kcross.wait_recv()
    k_pair = ring(KF, kz_send, kz_recv, 0)
    hand(KF, kp_send, kp_recv, z, k_order, k_hands)
    process(3)
    process(4)
    ship(2)

    pair[0].wait_recv()
    pair[1].wait_recv()
    pair = ring(QF, z_send, z_recv, 3)
    hand(QF, p_send, p_recv, (z + 5) % 8, order, hands)
    hand(QF, p_send, p_recv, (z + 3) % 8, order, hands)
    k_pair[0].wait_recv()
    k_pair[1].wait_recv()
    k_pair = ring(KF, kz_send, kz_recv, 1)
    hand(KF, kp_send, kp_recv, (z + 7) % 8, k_order, k_hands)
    hand(KF, kp_send, kp_recv, (z + 1) % 8, k_order, k_hands)
    process(5)
    process(6)
    ship(3)
    process_kv(0)

    k_pair[0].wait_recv()
    k_pair[1].wait_recv()
    k_pair = ring(KF, kz_send, kz_recv, 2)
    hand(KF, kp_send, kp_recv, (z + 6) % 8, k_order, k_hands)
    hand(KF, kp_send, kp_recv, (z + 2) % 8, k_order, k_hands)
    pair[0].wait_recv()
    pair[1].wait_recv()
    hand(QF, p_send, p_recv, (z + 4) % 8, order, hands)
    process_kv(1)
    process_kv(2)
    process(7)
    ship(4)

    k_pair[0].wait_recv()
    k_pair[1].wait_recv()
    k_pair = ring(KF, kz_send, kz_recv, 3)
    hand(KF, kp_send, kp_recv, (z + 5) % 8, k_order, k_hands)
    hand(KF, kp_send, kp_recv, (z + 3) % 8, k_order, k_hands)
    process_kv(3)
    process_kv(4)
    k_pair[0].wait_recv()
    k_pair[1].wait_recv()
    hand(KF, kp_send, kp_recv, (z + 4) % 8, k_order, k_hands)
    process_kv(5)
    process_kv(6)
    process_kv(7)

    @pl.loop(5, 8)
    def _(wp):
        @pl.when(wp != w)
        def _():
            chunk(wp).start()

    for h in range(2):
        ng_out[h * QB:(h + 1) * QB, :] = nacc[h].astype(jnp.bfloat16)
    FR[w] = F[pl.ds(6 * w, 6)]

    @pl.loop(0, 8)
    def _(ws):
        @pl.when(ws != w)
        def _():
            chunk_in(ws).wait_recv()

    for j in range(6):
        total = FR[0, j].astype(jnp.float32)
        for ws in range(1, 8):
            total += FR[ws, j].astype(jnp.float32)
        gw_out[:, j * 128:(j + 1) * 128] = total.astype(jnp.bfloat16)

    for c in sends + hands + k_hands:
        c.wait_send()

    @pl.loop(0, w + 1)
    def _(wp):
        first(wp).wait_send()

    second(w, 1 - xl).wait_send()

    @pl.loop(0, w)
    def _(wp):
        second(wp, 0).wait_send()
        second(wp, 1).wait_send()

    @pl.loop(0, 8)
    def _(wp):
        @pl.when(wp != w)
        def _():
            chunk(wp).wait_send()


def back(dq, dkv, normed, qkv_weight):
    vmem = pl.BlockSpec(memory_space=pltpu.VMEM)
    hbm = pl.BlockSpec(memory_space=pltpu.HBM)
    dma = pltpu.SemaphoreType.DMA
    low = jnp.bfloat16
    return pl.pallas_call(
        back_kernel,
        name="back",
        out_shape=(
            jax.ShapeDtypeStruct((512, 128), low),
            jax.ShapeDtypeStruct((128, 768), low),
        ),
        in_specs=[vmem, vmem, hbm, vmem],
        out_specs=(vmem, vmem),
        scratch_shapes=[
            pltpu.VMEM((2, 8, 2, QB, QB), low),
            pltpu.VMEM((2, 8, 2, QB, 128), low),
            pltpu.VMEM((8, QB, QB), low),
            pltpu.VMEM((8, 2, QB, 128), low),
            pltpu.VMEM((8, 2, QB, 128), low),
            pltpu.VMEM((48, 128, 128), low),
            pltpu.VMEM((8, 6, 128, 128), low),
            pltpu.VMEM((512, 128), low),
            pltpu.VMEM((2, QB, 128), jnp.float32),
            pltpu.VMEM((QB, 128), jnp.float32),
            dma((2,)), dma((8,)), dma((8,)), dma((8, 2)), dma((8, 2)), dma((2,)),
            dma((2, 4)), dma((2, 4)), dma((8,)), dma((8,)), dma((2,)), dma((2, 4)), dma((2, 4)),
            dma((8,)), dma((8,)), dma((8,)), dma((8,)),
        ],
        compiler_params=pltpu.CompilerParams(
            collective_id=1, has_side_effects=True, vmem_limit_bytes=40 * 1024 * 1024
        ),
        cost_estimate=pl.CostEstimate(flops=3_000_000_000, bytes_accessed=20_000_000, transcendentals=0),
    )(dq, dkv, normed, qkv_weight)


def local(
    normed, queries, keys, values, attn_out, row_logsumexp, out_grad, out_weight, qkv_weight, documents, tasks
):
    attn_grad, kv, part = front(out_grad, out_weight, keys, values, attn_out)
    arrived = lax.all_to_all(part, "wide", split_axis=0, concat_axis=0, tiled=True)
    dq, dkv = attend(
        documents, queries, attn_grad, attn_out, row_logsumexp, kv.reshape(2, BLOCKS, QB, 128)
    )
    normed_grad, qkv_sum = back(dq, dkv, normed, qkv_weight)
    out_sum = arrived.astype(jnp.float32).sum(axis=0).astype(jnp.bfloat16)
    return normed_grad, out_sum, qkv_sum


def solution(mesh):
    in_specs = (
        P("wide", ("role", "tp")),
        P("wide", "tp"),
        P("wide", None),
        P("wide", None),
        P("wide", "tp"),
        P("tp", None),
        P("wide", ("role", "tp")),
        P("tp", None),
        P(("role", "tp"), None),
        P(),
        P(),
    )
    out_specs = (P("wide", ("role", "tp")), P("tp", ("role", "wide")), P(("role", "tp"), "wide"))
    return jax.shard_map(local, mesh=mesh, in_specs=in_specs, out_specs=out_specs, check_vma=False)
```

```python
import jax
import jax.numpy as jnp
from jax import lax
from jax.experimental import pallas as pl
from jax.experimental.pallas import tpu as pltpu
from jax.sharding import PartitionSpec as P

MESH = pl.DeviceIdType.MESH
D = 4096
HEAD_SIZE = 128
QB = 256
LOG2E = 1.4426950408889634
SCALE = HEAD_SIZE ** (-0.5)
NT = (((1,), (1,)), ((), ()))
TN = (((0,), (0,)), ((), ()))
NN = (((1,), (0,)), ((), ()))


def dot(a, b, dims):
    return lax.dot_general(a, b, dims, preferred_element_type=jnp.float32)


def aligned(at, size):
    return pl.ds(pl.multiple_of(at * size, size), size)


def remote(src, dst, send, recv, where):
    return pltpu.make_async_remote_copy(
        src_ref=src, dst_ref=dst, send_sem=send, recv_sem=recv, device_id=where, device_id_type=MESH
    )


def greet(places):
    barrier = pltpu.get_barrier_semaphore()
    for where in places:
        pl.semaphore_signal(barrier, inc=1, device_id=where, device_id_type=MESH)
    pl.semaphore_wait(barrier, len(places))


def place():
    r = lax.axis_index("role")
    w = lax.axis_index("wide")
    t = lax.axis_index("tp")
    return r, w, t, t // 2, t % 2


def plane_peer(w, z, xl, k):
    dx, dy = k // 4, k % 4
    peer = ((w // 4 + dx) % 2) * 4 + (w % 4 + dy) % 4
    return {"wide": peer, "tp": z * 2 + (xl if dx == 0 else 1 - xl)}


class Gather:
    def __init__(self, block, zs, zr, xs, xr):
        self.block, self.zs, self.zr, self.xs, self.xr = block, zs, zr, xs, xr
        r, w, t, self.z, self.xl = place()
        self.ways = (
            {"tp": ((self.z + 1) % 8) * 2 + self.xl},
            {"tp": ((self.z + 7) % 8) * 2 + self.xl},
        )
        self.inner = {"tp": self.z * 2 + 1 - self.xl}
        self.sent, self.hops, self.crossed = [], {}, {}

    def at(self, d, s):
        return (self.z + 8 - s) % 8 if d == 0 else (self.z + s) % 8

    def piece(self, at, j, share=None):
        if j < 2:
            return self.block(at, self.xl, 128 * j, 128)
        if share is None:
            return self.block(at, 1 - self.xl, 0, 128)
        return self.block(at, 1 - self.xl, 64 * share, 64)

    def go(self, ref, send, recv, where):
        c = remote(ref, ref, send, recv, where)
        c.start()
        self.sent.append(c)
        return c

    def hop(self, d, s, j):
        ref = self.piece(self.at(d, s), j, d if s == 3 else None)
        self.hops[d, s, j] = self.go(ref, self.zs.at[d, s, j], self.zr.at[d, s, j], self.ways[d])

    def cross(self, at, j, k):
        self.crossed[k] = self.go(self.piece(at, j), self.xs.at[k], self.xr.at[k], self.inner)

    def start(self):
        for j in range(2):
            self.hop(0, 0, j)
            self.hop(1, 0, j)
            self.cross(self.z, j, 8 if j == 0 else 0)

    def second(self):
        self.crossed[8].wait_recv()
        self.hop(0, 0, 2)
        self.hop(1, 0, 2)

    def step(self, s, j):
        for d in range(2):
            if s == 4 and j < 2 and d != j:
                continue
            self.hops[d, s - 1, j].wait_recv()
            if s < 3 or (s == 3 and (j == 2 or d == j)):
                self.hop(d, s, j)
            if j == 1:
                self.cross(self.at(d, s), 1, 7 if s == 4 else 2 * s - 1 + d)

    def whole(self, s):
        for k in ((0,), (1, 2), (3, 4), (5, 6), (7,))[s]:
            self.crossed[k].wait_recv()

    def blocks(self, s):
        return ((self.z + 8 - s) % 8, (self.z + s) % 8) if s in (1, 2, 3) else ((self.z + s) % 8,)

    def finish(self):
        for c in self.sent:
            c.wait_send()


def count_below(docs, value):
    below = jnp.where(docs < value, 1.0, 0.0)
    count = jnp.sum(jnp.sum(below, axis=0, keepdims=True), axis=1, keepdims=True)
    return count.astype(jnp.int32)


def whole_kernel(
    normed, queries, keys, values, ao, lse_in, og, ow, wq_in, docs_in,
    ng_out, ow_out, gw_out,
    docs, G, O, W, AO, OP, OR, acc, kv, Q, lse, q2, g2, dq, dqb, dkv,
    QF, KF, D1, S, D2, F, FR, N, wq, nacc, kacc,
    lsem, swap_sem, k_send, k_recv, kp_sem, ao_sem, aoh_sem, n_sem, o_send, o_recv,
    az_s, az_r, ax_s, ax_r, ah_s, ah_r,
    ez_s, ez_r, ex_s, ex_r, eh_s, eh_r,
    vz_s, vz_r, vx_s, vx_r, vh_s, vh_r,
    d1s, d1r, d2s, d2r, f_send, f_recv,
):
    r, w, t, z, xl = place()
    low = jnp.bfloat16
    partner = {"role": 1 - r}
    inner = {"tp": z * 2 + 1 - xl}
    up = {"tp": ((z + 1) % 8) * 2 + xl}
    down = {"tp": ((z + 7) % 8) * 2 + xl}
    plane = [{"wide": (w + k // 2) % 8, "tp": z * 2 + (xl + k % 2) % 2} for k in range(1, 16)]
    cols = aligned(xl, 128)
    mine = aligned(r, QB)
    other = aligned(1 - r, QB)
    heads = aligned(z, 128)

    @pl.when(r == 0)
    def _():
        pltpu.make_async_copy(keys.at[:, heads], kv.at[r, w], lsem.at[0]).start()

    @pl.when(r == 1)
    def _():
        pltpu.make_async_copy(values.at[:, heads], kv.at[r, w], lsem.at[0]).start()

    load_own = pltpu.make_async_copy(og.at[mine, :], G.at[z, r, :, cols], lsem.at[1])
    load_ao = pltpu.make_async_copy(ao, AO.at[0], lsem.at[2])
    load_w = pltpu.make_async_copy(ow, W, lsem.at[3])
    load_docs = pltpu.make_async_copy(docs_in, docs, lsem.at[4])
    load_q = pltpu.make_async_copy(queries.at[mine, :], Q, lsem.at[5])
    load_lse = pltpu.make_async_copy(lse_in, lse, lsem.at[6])
    load_n = pltpu.make_async_copy(normed, N.at[0], lsem.at[7])
    load_wq = pltpu.make_async_copy(wq_in, wq, lsem.at[8])
    for c in (load_own, load_ao, load_w, load_docs, load_q, load_lse, load_n, load_wq):
        c.start()

    greet([partner, up, down] + plane)

    swap = remote(
        og.at[other, :], G.at[z, r, :, cols], swap_sem.at[0], swap_sem.at[1], partner
    )
    swap.start()
    sends = [swap]
    load_ao.wait()
    lend = remote(AO.at[0, mine], AO.at[1, mine], ao_sem.at[0], ao_sem.at[1], inner)
    lend.start()
    sends.append(lend)
    pltpu.make_async_copy(keys.at[:, heads], kv.at[r, w], lsem.at[0]).wait()
    pushes = []
    for k in range(1, 8):
        c = remote(
            kv.at[r, w], kv.at[r, w], k_send.at[k - 1], k_recv.at[k - 1], plane_peer(w, z, xl, k)
        )
        c.start()
        pushes.append(c)
    load_own.wait()
    swap.wait_recv()

    A = Gather(
        lambda at, x, row, n: G.at[at, :, pl.ds(row, n), aligned(x, 128)], az_s, az_r, ax_s, ax_r
    )
    A.start()
    load_w.wait()
    acc[...] = jnp.zeros_like(acc)
    A.second()

    order, hands = [], []

    def give(at):
        k = len(order)
        c = remote(G.at[at, 1 - r], O.at[at], ah_s.at[k], ah_r.at[k], partner)
        c.start()
        order.append(at)
        hands.append(c)

    def use(at):
        low_cols = aligned(at, QB)
        high_cols = aligned(at + 8, QB)
        acc[...] += dot(G[at, 0], W[:, low_cols], NT) + dot(G[at, 1], W[:, high_cols], NT)

    def out_chunk(at):
        far = (at // 4 + w // 4) % 2
        return remote(
            OP.at[at], OR.at[w], o_send.at[at], o_recv.at[w],
            {"wide": at, "tp": z * 2 + (xl + far) % 2},
        )

    def product(k):
        at = order[k]
        far = (at // 4 + w // 4) % 2
        hands[k].wait_recv()
        total = dot(AO[far, mine, :], G[at, r], TN) + dot(AO[far, other, :], O[at], TN)
        OP[at] = total.astype(low)

        @pl.when(at != w)
        def _():
            out_chunk(at).start()

    def whole(s):
        A.whole(s)
        for at in A.blocks(s):
            give(at)

    A.step(1, 0)
    A.step(1, 1)
    lend.wait_recv()
    lent = remote(AO.at[1, mine], AO.at[1, mine], aoh_sem.at[0], aoh_sem.at[1], partner)
    lent.start()
    sends.append(lent)
    A.step(1, 2)
    whole(0)
    lent.wait_recv()
    A.step(2, 0)
    A.step(2, 1)
    use(order[0])
    product(0)
    A.step(2, 2)
    whole(1)
    A.step(3, 0)
    use(order[1])
    A.step(3, 1)
    use(order[2])
    product(1)
    A.step(3, 2)
    product(2)
    whole(2)
    A.step(4, 0)
    use(order[3])
    product(3)
    A.step(4, 1)
    use(order[4])
    product(4)
    for c in pushes:
        c.wait_recv()
    hand_kv = remote(kv.at[r], kv.at[r], kp_sem.at[0], kp_sem.at[1], partner)
    hand_kv.start()
    sends.append(hand_kv)
    A.step(4, 2)
    whole(3)
    use(order[5])
    use(order[6])
    whole(4)
    use(order[7])

    load_n.wait()
    lend_n = remote(N.at[0], N.at[1], n_sem.at[0], n_sem.at[1], inner)
    lend_n.start()
    sends.append(lend_n)
    load_docs.wait()
    load_q.wait()
    load_lse.wait()
    start_at = (2 * w + r) * QB
    c1 = count_below(docs[...], 1)
    c2 = count_below(docs[...], 2)
    span = aligned(2 * w + r, QB)
    deltas, lses = [], []
    for h in range(2):
        hc = pl.ds(h * 128, 128)
        q2[pl.ds(h * QB, QB), :] = Q[:, hc]
        g = acc[:, hc].astype(low)
        g2[pl.ds(h * QB, QB), :] = g
        both = g.astype(jnp.float32) * AO[0, mine, hc].astype(jnp.float32)
        deltas.append(jnp.sum(both.T, axis=0, keepdims=True))
        lses.append(lse[pl.ds(h, 1), span] * LOG2E)
    delta = jnp.concatenate(deltas, axis=1)
    lse2 = jnp.concatenate(lses, axis=1)
    lane = lax.broadcasted_iota(jnp.int32, (1, 2 * QB), 1)
    q_pos = start_at + jnp.where(lane >= QB, lane - QB, lane)
    q_start = jnp.where(q_pos >= c2, c2, jnp.where(q_pos >= c1, c1, 0))
    dq[...] = jnp.zeros_like(dq)
    product(5)
    product(6)
    product(7)
    hand_kv.wait_recv()

    def first(wp):
        return remote(dkv.at[wp, 1 - r], D1.at[wp], d1s.at[wp], d1r.at[wp], partner)

    def second(wp, kind):
        return remote(
            S.at[wp, kind], D2.at[w, xl], d2s.at[wp, kind], d2r.at[w, xl],
            {"wide": wp, "tp": z * 2 + kind},
        )

    def arrive(ws, xs):
        return remote(
            S.at[w, xl], D2.at[ws, xs], d2s.at[w, xl], d2r.at[ws, xs],
            {"wide": ws, "tp": z * 2 + xs},
        )

    def pair_sum(wp):
        first(wp).wait_recv()
        both = (dkv[wp, r].astype(jnp.float32) + D1[wp].astype(jnp.float32)).astype(low)
        S[wp, 0] = both[:, 0:128]
        S[wp, 1] = both[:, 128:256]

    @pl.loop(0, w + 1)
    def _(i):
        k_rows = kv[0, i]
        v_rows = kv[1, i]
        scores = dot(k_rows, q2[...], NT)
        k_pos = i * 512 + lax.broadcasted_iota(jnp.int32, (512, 1), 0)
        allowed = (k_pos <= q_pos) & (k_pos >= q_start)
        probs = jnp.where(allowed, jnp.exp2(scores * (SCALE * LOG2E) - lse2), 0.0)
        dv = dot(probs.astype(low), g2[...], NN).astype(low)
        prob_grad = dot(v_rows, g2[...], NT)
        ds = (probs * (prob_grad - delta)).astype(low)
        dk = (dot(ds, q2[...], NN) * SCALE).astype(low)
        dq[...] += dot(ds, k_rows, TN)
        for h in range(2):
            dkv[i, h, :, 0:128] = dk[h * QB:(h + 1) * QB, :]
            dkv[i, h, :, 128:256] = dv[h * QB:(h + 1) * QB, :]
        first(i).start()

        @pl.when(i > 0)
        def _():
            pair_sum(i - 1)
            second(i - 1, 0).start()
            second(i - 1, 1).start()

    for h in range(2):
        dqb[:, h * 128:(h + 1) * 128] = (dq[pl.ds(h * QB, QB), :] * SCALE).astype(low)
    QF[r, z, xl] = dqb[...]
    pair_sum(w)
    second(w, 1 - xl).start()

    E = Gather(lambda at, x, row, n: QF.at[r, at, x, pl.ds(row, n), :], ez_s, ez_r, ex_s, ex_r)
    V = Gather(lambda at, x, row, n: KF.at[r, at, x, pl.ds(row, n), :], vz_s, vz_r, vx_s, vx_r)
    E.start()
    load_wq.wait()
    nacc[...] = jnp.zeros_like(nacc)

    E.second()

    def key_sums():
        kacc[...] = S[w, xl].astype(jnp.float32)

        @pl.loop(w + 1, 8)
        def _(ws):
            for xs in range(2):
                arrive(ws, xs).wait_recv()
                kacc[...] += D2[ws, xs].astype(jnp.float32)

        arrive(w, 1 - xl).wait_recv()
        KF[r, z, xl] = (kacc[...] + D2[w, 1 - xl].astype(jnp.float32)).astype(low)

    e_order, e_hands, v_order, v_hands = [], [], [], []

    def pass_on(gather, s, buf, ss, rs, seen, copies):
        gather.whole(s)
        for at in gather.blocks(s):
            k = len(seen)
            c = remote(buf.at[r, at], buf.at[r, at], ss.at[k], rs.at[k], partner)
            c.start()
            seen.append(at)
            copies.append(c)

    def e_whole(s):
        pass_on(E, s, QF, eh_s, eh_r, e_order, e_hands)

    def v_whole(s):
        pass_on(V, s, KF, vh_s, vh_r, v_order, v_hands)

    def process(k):
        at = e_order[k]
        e_hands[k].wait_recv()
        for x in range(2):
            weight = wq[:, aligned(2 * at + x, QB)]
            far = (((2 * at + x) // 3) // 4 + w // 4) % 2
            for h in range(2):
                nacc[h] += dot(QF[h, at, x], weight, NT)
            total = dot(N[far, 0:QB, :], QF[0, at, x], TN) + dot(N[far, QB:512, :], QF[1, at, x], TN)
            F[4 * at + 2 * x] = total[:, 0:128].astype(low)
            F[4 * at + 2 * x + 1] = total[:, 128:256].astype(low)

            @pl.when((2 * at + x) // 3 != w)
            def _():
                two(2 * at + x).start()

    def process_kv(k):
        at = v_order[k]
        v_hands[k].wait_recv()
        for x in range(2):
            spot = 32 + 8 * x + at
            weight = wq[:, aligned(spot, 128)]
            far = ((spot // 6) // 4 + w // 4) % 2
            for h in range(2):
                nacc[h] += dot(KF[h, at, x], weight, NT)
            total = dot(N[far, 0:QB, :], KF[0, at, x], TN) + dot(N[far, QB:512, :], KF[1, at, x], TN)
            F[spot] = total.astype(low)

            @pl.when(spot // 6 != w)
            def _():
                one(spot).start()

    def peer(wp):
        far = (wp // 4 + w // 4) % 2
        return {"wide": wp, "tp": z * 2 + (xl + far) % 2}

    def two(tp):
        return remote(
            F.at[pl.ds(2 * tp, 2)], FR.at[w, pl.ds(2 * (tp % 3), 2)],
            f_send.at[2 * tp], f_recv.at[w, 2 * (tp % 3)], peer(tp // 3),
        )

    def one(spot):
        return remote(
            F.at[spot], FR.at[w, spot % 6], f_send.at[spot], f_recv.at[w, spot % 6], peer(spot // 6)
        )

    def two_in(ws, j):
        return remote(
            F.at[pl.ds(6 * w + 2 * j, 2)], FR.at[ws, pl.ds(2 * j, 2)],
            f_send.at[6 * w + 2 * j], f_recv.at[ws, 2 * j], peer(ws),
        )

    def one_in(ws, j):
        return remote(F.at[6 * w + j], FR.at[ws, j], f_send.at[6 * w + j], f_recv.at[ws, j], peer(ws))

    E.step(1, 0)
    lend_n.wait_recv()
    E.step(1, 1)
    key_sums()
    V.start()
    E.step(1, 2)
    V.second()
    e_whole(0)
    E.step(2, 0)
    E.step(2, 1)
    V.step(1, 0)
    V.step(1, 1)
    process(0)
    E.step(2, 2)
    V.step(1, 2)
    e_whole(1)
    v_whole(0)
    E.step(3, 0)
    process(1)
    E.step(3, 1)
    V.step(2, 0)
    V.step(2, 1)
    process(2)
    E.step(3, 2)
    V.step(2, 2)
    process_kv(0)
    e_whole(2)
    v_whole(1)
    E.step(4, 0)
    process(3)
    E.step(4, 1)
    V.step(3, 0)
    V.step(3, 1)
    process(4)
    E.step(4, 2)
    V.step(3, 2)
    process_kv(1)
    process_kv(2)
    e_whole(3)
    v_whole(2)
    process(5)
    process(6)
    e_whole(4)
    V.step(4, 0)
    V.step(4, 1)
    V.step(4, 2)
    process_kv(3)
    process_kv(4)
    process(7)
    v_whole(3)
    v_whole(4)
    process_kv(5)
    process_kv(6)
    process_kv(7)

    for h in range(2):
        ng_out[h * QB:(h + 1) * QB, :] = nacc[h].astype(low)

    OR[w] = OP[w]

    @pl.loop(0, 8)
    def _(ws):
        @pl.when(ws != w)
        def _():
            far = (ws // 4 + w // 4) % 2
            remote(
                OP.at[w], OR.at[ws], o_send.at[w], o_recv.at[ws],
                {"wide": ws, "tp": z * 2 + (xl + far) % 2},
            ).wait_recv()

    total = OR[0].astype(jnp.float32)
    for ws in range(1, 8):
        total += OR[ws].astype(jnp.float32)
    ow_out[...] = total.astype(low)

    FR[w] = F[pl.ds(6 * w, 6)]

    @pl.loop(0, 8)
    def _(ws):
        @pl.when(ws != w)
        def _():
            for j in range(3):
                @pl.when((w < 5) | ((w == 5) & (j == 0)))
                def _():
                    two_in(ws, j).wait_recv()

            for j in range(6):
                @pl.when((w > 5) | ((w == 5) & (j > 1)))
                def _():
                    one_in(ws, j).wait_recv()

    for j in range(6):
        total = FR[0, j].astype(jnp.float32)
        for ws in range(1, 8):
            total += FR[ws, j].astype(jnp.float32)
        gw_out[:, j * 128:(j + 1) * 128] = total.astype(low)

    for c in sends + pushes + hands + e_hands + v_hands:
        c.wait_send()
    for gather in (A, E, V):
        gather.finish()

    @pl.loop(0, w)
    def _(wp):
        first(wp).wait_send()
        second(wp, 0).wait_send()
        second(wp, 1).wait_send()

    first(w).wait_send()
    second(w, 1 - xl).wait_send()

    @pl.loop(0, 8)
    def _(wp):
        @pl.when(wp != w)
        def _():
            out_chunk(wp).wait_send()

    @pl.loop(0, 16)
    def _(tp):
        @pl.when(tp // 3 != w)
        def _():
            two(tp).wait_send()

        @pl.when((32 + tp) // 6 != w)
        def _():
            one(32 + tp).wait_send()


def local(
    normed, queries, keys, values, attn_out, row_logsumexp, out_grad, out_weight, qkv_weight, documents, tasks
):
    hbm = pl.BlockSpec(memory_space=pltpu.HBM)
    vmem = pl.BlockSpec(memory_space=pltpu.VMEM)
    dma = pltpu.SemaphoreType.DMA
    low, wide = jnp.bfloat16, jnp.float32
    ring = [dma((2, 4, 3)), dma((2, 4, 3)), dma((9,)), dma((9,)), dma((8,)), dma((8,))]
    return pl.pallas_call(
        whole_kernel,
        name="layer",
        out_shape=(
            jax.ShapeDtypeStruct((512, 128), low),
            jax.ShapeDtypeStruct((QB, QB), low),
            jax.ShapeDtypeStruct((128, 768), low),
        ),
        in_specs=[hbm] * 10,
        out_specs=(vmem, vmem, vmem),
        scratch_shapes=[
            pltpu.VMEM((32, 128), jnp.int32),
            pltpu.VMEM((8, 2, QB, QB), low),
            pltpu.VMEM((8, QB, QB), low),
            pltpu.VMEM((QB, D), low),
            pltpu.VMEM((2, 512, QB), low),
            pltpu.VMEM((8, QB, QB), low),
            pltpu.VMEM((8, QB, QB), low),
            pltpu.VMEM((QB, QB), wide),
            pltpu.VMEM((2, 8, 512, 128), low),
            pltpu.VMEM((QB, QB), low),
            pltpu.VMEM((2, 4096), wide),
            pltpu.VMEM((512, 128), low),
            pltpu.VMEM((512, 128), low),
            pltpu.VMEM((512, 128), wide),
            pltpu.VMEM((QB, QB), low),
            pltpu.VMEM((8, 2, QB, QB), low),
            pltpu.VMEM((2, 8, 2, QB, QB), low),
            pltpu.VMEM((2, 8, 2, QB, 128), low),
            pltpu.VMEM((8, QB, QB), low),
            pltpu.VMEM((8, 2, QB, 128), low),
            pltpu.VMEM((8, 2, QB, 128), low),
            pltpu.VMEM((48, 128, 128), low),
            pltpu.VMEM((8, 6, 128, 128), low),
            pltpu.VMEM((2, 512, 128), low),
            pltpu.VMEM((128, 6144), low),
            pltpu.VMEM((2, QB, 128), wide),
            pltpu.VMEM((QB, 128), wide),
            dma((9,)), dma((2,)), dma((7,)), dma((7,)), dma((2,)), dma((2,)), dma((2,)), dma((2,)),
            dma((8,)), dma((8,)),
        ]
        + ring * 3
        + [dma((8,)), dma((8,)), dma((8, 2)), dma((8, 2)), dma((48,)), dma((8, 6))],
        compiler_params=pltpu.CompilerParams(
            collective_id=0, has_side_effects=True, vmem_limit_bytes=60 * 1024 * 1024
        ),
        cost_estimate=pl.CostEstimate(
            flops=10_000_000_000, bytes_accessed=40_000_000, transcendentals=2_000_000
        ),
    )(
        normed, queries, keys, values, attn_out, row_logsumexp, out_grad, out_weight, qkv_weight,
        documents.reshape(32, 128),
    )


def solution(mesh):
    in_specs = (
        P("wide", ("role", "tp")),
        P("wide", "tp"),
        P("wide", None),
        P("wide", None),
        P("wide", "tp"),
        P("tp", None),
        P("wide", ("role", "tp")),
        P("tp", None),
        P(("role", "tp"), None),
        P(),
        P(),
    )
    out_specs = (P("wide", ("role", "tp")), P("tp", ("role", "wide")), P(("role", "tp"), "wide"))
    return jax.shard_map(local, mesh=mesh, in_specs=in_specs, out_specs=out_specs, check_vma=False)
```

```python
import jax
import jax.numpy as jnp
from jax import lax
from jax.experimental import pallas as pl
from jax.experimental.pallas import tpu as pltpu
from jax.sharding import PartitionSpec as P

MESH = pl.DeviceIdType.MESH
D = 4096
HEAD_SIZE = 128
QB = 256
LOG2E = 1.4426950408889634
SCALE = HEAD_SIZE ** (-0.5)
NT = (((1,), (1,)), ((), ()))
TN = (((0,), (0,)), ((), ()))
NN = (((1,), (0,)), ((), ()))


def dot(a, b, dims):
    return lax.dot_general(a, b, dims, preferred_element_type=jnp.float32)


def aligned(at, size):
    return pl.ds(pl.multiple_of(at * size, size), size)


def remote(src, dst, send, recv, where):
    return pltpu.make_async_remote_copy(
        src_ref=src, dst_ref=dst, send_sem=send, recv_sem=recv, device_id=where, device_id_type=MESH
    )


def greet(places):
    barrier = pltpu.get_barrier_semaphore()
    for where in places:
        pl.semaphore_signal(barrier, inc=1, device_id=where, device_id_type=MESH)
    pl.semaphore_wait(barrier, len(places))


def place():
    r = lax.axis_index("role")
    w = lax.axis_index("wide")
    t = lax.axis_index("tp")
    return r, w, t, t // 2, t % 2


def plane_peer(w, z, xl, k):
    dx, dy = k // 4, k % 4
    peer = ((w // 4 + dx) % 2) * 4 + (w % 4 + dy) % 4
    return {"wide": peer, "tp": z * 2 + (xl if dx == 0 else 1 - xl)}


class Gather:
    def __init__(self, block, zs, zr, xs, xr):
        self.block, self.zs, self.zr, self.xs, self.xr = block, zs, zr, xs, xr
        r, w, t, self.z, self.xl = place()
        self.ways = (
            {"tp": ((self.z + 1) % 8) * 2 + self.xl},
            {"tp": ((self.z + 7) % 8) * 2 + self.xl},
        )
        self.inner = {"tp": self.z * 2 + 1 - self.xl}
        self.sent, self.hops, self.crossed = [], {}, {}

    def at(self, d, s):
        return (self.z + 8 - s) % 8 if d == 0 else (self.z + s) % 8

    def piece(self, at, j, share=None):
        if j < 2:
            return self.block(at, self.xl, 128 * j, 128)
        if share is None:
            return self.block(at, 1 - self.xl, 0, 128)
        return self.block(at, 1 - self.xl, 64 * share, 64)

    def go(self, ref, send, recv, where):
        c = remote(ref, ref, send, recv, where)
        c.start()
        self.sent.append(c)
        return c

    def hop(self, d, s, j):
        ref = self.piece(self.at(d, s), j, d if s == 3 else None)
        self.hops[d, s, j] = self.go(ref, self.zs.at[d, s, j], self.zr.at[d, s, j], self.ways[d])

    def cross(self, at, j, k):
        self.crossed[k] = self.go(self.piece(at, j), self.xs.at[k], self.xr.at[k], self.inner)

    def start(self):
        for j in range(2):
            self.hop(0, 0, j)
            self.hop(1, 0, j)
            self.cross(self.z, j, 8 if j == 0 else 0)

    def second(self):
        self.crossed[8].wait_recv()
        self.hop(0, 0, 2)
        self.hop(1, 0, 2)

    def step(self, s, j):
        for d in range(2):
            if s == 4 and j < 2 and d != j:
                continue
            self.hops[d, s - 1, j].wait_recv()
            if s < 3 or (s == 3 and (j == 2 or d == j)):
                self.hop(d, s, j)
            if j == 1:
                self.cross(self.at(d, s), 1, 7 if s == 4 else 2 * s - 1 + d)

    def whole(self, s):
        for k in ((0,), (1, 2), (3, 4), (5, 6), (7,))[s]:
            self.crossed[k].wait_recv()

    def blocks(self, s):
        return ((self.z + 8 - s) % 8, (self.z + s) % 8) if s in (1, 2, 3) else ((self.z + s) % 8,)

    def finish(self):
        for c in self.sent:
            c.wait_send()


def count_below(docs, value):
    below = jnp.where(docs < value, 1.0, 0.0)
    count = jnp.sum(jnp.sum(below, axis=0, keepdims=True), axis=1, keepdims=True)
    return count.astype(jnp.int32)


def whole_kernel(
    normed, queries, keys, values, ao, lse_in, og, ow, wq_in, docs_in,
    ng_out, ow_out, gw_out,
    docs, G, O, W, AO, OP, OX, OR, acc, kv, Q, lse, q2, g2, dq, dqb, dkv,
    QF, KF, D1, S, D2, F, FX, FR, N, wq, nacc, kacc,
    lsem, swap_sem, k_send, k_recv, kp_sem, ao_sem, aoh_sem, n_sem, o_send, ox_recv, o_recv,
    az_s, az_r, ax_s, ax_r, ah_s, ah_r,
    ez_s, ez_r, ex_s, ex_r, eh_s, eh_r,
    vz_s, vz_r, vx_s, vx_r, vh_s, vh_r,
    d1s, d1r, d2s, d2r, f_send, fx_recv, f_recv,
):
    r, w, t, z, xl = place()
    low = jnp.bfloat16
    partner = {"role": 1 - r}
    inner = {"tp": z * 2 + 1 - xl}
    outer = {"wide": (w + 4) % 8, "tp": z * 2 + 1 - xl}
    side = w % 4
    up = {"tp": ((z + 1) % 8) * 2 + xl}
    down = {"tp": ((z + 7) % 8) * 2 + xl}
    plane = [{"wide": (w + k // 2) % 8, "tp": z * 2 + (xl + k % 2) % 2} for k in range(1, 16)]
    cols = aligned(xl, 128)
    mine = aligned(r, QB)
    other = aligned(1 - r, QB)
    heads = aligned(z, 128)

    @pl.when(r == 0)
    def _():
        pltpu.make_async_copy(keys.at[:, heads], kv.at[r, w], lsem.at[0]).start()

    @pl.when(r == 1)
    def _():
        pltpu.make_async_copy(values.at[:, heads], kv.at[r, w], lsem.at[0]).start()

    load_own = pltpu.make_async_copy(og.at[mine, :], G.at[z, r, :, cols], lsem.at[1])
    load_ao = pltpu.make_async_copy(ao, AO.at[0], lsem.at[2])
    load_w = pltpu.make_async_copy(ow, W, lsem.at[3])
    load_docs = pltpu.make_async_copy(docs_in, docs, lsem.at[4])
    load_q = pltpu.make_async_copy(queries.at[mine, :], Q, lsem.at[5])
    load_lse = pltpu.make_async_copy(lse_in, lse, lsem.at[6])
    load_n = pltpu.make_async_copy(normed, N.at[0], lsem.at[7])
    load_wq = pltpu.make_async_copy(wq_in, wq, lsem.at[8])
    for c in (load_own, load_ao, load_w, load_docs, load_q, load_lse, load_n, load_wq):
        c.start()

    greet([partner, up, down] + plane)

    swap = remote(
        og.at[other, :], G.at[z, r, :, cols], swap_sem.at[0], swap_sem.at[1], partner
    )
    swap.start()
    sends = [swap]
    load_ao.wait()
    lend = remote(AO.at[0, mine], AO.at[1, mine], ao_sem.at[0], ao_sem.at[1], inner)
    lend.start()
    sends.append(lend)
    pltpu.make_async_copy(keys.at[:, heads], kv.at[r, w], lsem.at[0]).wait()
    pushes = []
    for k in range(1, 8):
        c = remote(
            kv.at[r, w], kv.at[r, w], k_send.at[k - 1], k_recv.at[k - 1], plane_peer(w, z, xl, k)
        )
        c.start()
        pushes.append(c)
    load_own.wait()
    swap.wait_recv()

    A = Gather(
        lambda at, x, row, n: G.at[at, :, pl.ds(row, n), aligned(x, 128)], az_s, az_r, ax_s, ax_r
    )
    A.start()
    load_w.wait()
    acc[...] = jnp.zeros_like(acc)
    A.second()

    order, hands = [], []

    def give(at):
        k = len(order)
        c = remote(G.at[at, 1 - r], O.at[at], ah_s.at[k], ah_r.at[k], partner)
        c.start()
        order.append(at)
        hands.append(c)

    def use(at):
        low_cols = aligned(at, QB)
        high_cols = aligned(at + 8, QB)
        acc[...] += dot(G[at, 0], W[:, low_cols], NT) + dot(G[at, 1], W[:, high_cols], NT)

    def across(wp):
        return (wp // 4 + w // 4) % 2

    def out_cross(at):
        return remote(OP.at[at], OX.at[at], o_send.at[at], ox_recv.at[at], outer)

    def out_chunk(at):
        return remote(OP.at[at], OR.at[side], o_send.at[at], o_recv.at[side], {"wide": at})

    def product(k):
        at = order[k]
        far = across(at)
        hands[k].wait_recv()
        total = dot(AO[far, mine, :], G[at, r], TN) + dot(AO[far, other, :], O[at], TN)
        OP[at] = total.astype(low)

        @pl.when(far == 1)
        def _():
            out_cross(at).start()

    def out_merge(k):
        at = order[k]

        @pl.when(across(at) == 0)
        def _():
            out_cross(at).wait_recv()
            OP[at] = (OP[at].astype(jnp.float32) + OX[at].astype(jnp.float32)).astype(low)

        @pl.when((across(at) == 0) & (at != w))
        def _():
            out_chunk(at).start()

    def whole(s):
        A.whole(s)
        for at in A.blocks(s):
            give(at)

    A.step(1, 0)
    A.step(1, 1)
    lend.wait_recv()
    lent = remote(AO.at[1, mine], AO.at[1, mine], aoh_sem.at[0], aoh_sem.at[1], partner)
    lent.start()
    sends.append(lent)
    A.step(1, 2)
    whole(0)
    lent.wait_recv()
    A.step(2, 0)
    A.step(2, 1)
    use(order[0])
    product(0)
    A.step(2, 2)
    whole(1)
    A.step(3, 0)
    use(order[1])
    A.step(3, 1)
    use(order[2])
    product(1)
    A.step(3, 2)
    product(2)
    out_merge(0)
    whole(2)
    A.step(4, 0)
    use(order[3])
    product(3)
    A.step(4, 1)
    use(order[4])
    product(4)
    out_merge(1)
    out_merge(2)
    for c in pushes:
        c.wait_recv()
    hand_kv = remote(kv.at[r], kv.at[r], kp_sem.at[0], kp_sem.at[1], partner)
    hand_kv.start()
    sends.append(hand_kv)
    A.step(4, 2)
    whole(3)
    use(order[5])
    use(order[6])
    whole(4)
    use(order[7])

    load_n.wait()
    lend_n = remote(N.at[0], N.at[1], n_sem.at[0], n_sem.at[1], inner)
    lend_n.start()
    sends.append(lend_n)
    load_docs.wait()
    load_q.wait()
    load_lse.wait()
    start_at = (2 * w + r) * QB
    c1 = count_below(docs[...], 1)
    c2 = count_below(docs[...], 2)
    span = aligned(2 * w + r, QB)
    deltas, lses = [], []
    for h in range(2):
        hc = pl.ds(h * 128, 128)
        q2[pl.ds(h * QB, QB), :] = Q[:, hc]
        g = acc[:, hc].astype(low)
        g2[pl.ds(h * QB, QB), :] = g
        both = g.astype(jnp.float32) * AO[0, mine, hc].astype(jnp.float32)
        deltas.append(jnp.sum(both.T, axis=0, keepdims=True))
        lses.append(lse[pl.ds(h, 1), span] * LOG2E)
    delta = jnp.concatenate(deltas, axis=1)
    lse2 = jnp.concatenate(lses, axis=1)
    lane = lax.broadcasted_iota(jnp.int32, (1, 2 * QB), 1)
    q_pos = start_at + jnp.where(lane >= QB, lane - QB, lane)
    q_start = jnp.where(q_pos >= c2, c2, jnp.where(q_pos >= c1, c1, 0))
    dq[...] = jnp.zeros_like(dq)
    product(5)
    product(6)
    product(7)
    out_merge(3)
    out_merge(4)
    hand_kv.wait_recv()

    def first(wp):
        return remote(dkv.at[wp, 1 - r], D1.at[wp], d1s.at[wp], d1r.at[wp], partner)

    def second(wp, kind):
        return remote(
            S.at[wp, kind], D2.at[w, xl], d2s.at[wp, kind], d2r.at[w, xl],
            {"wide": wp, "tp": z * 2 + kind},
        )

    def arrive(ws, xs):
        return remote(
            S.at[w, xl], D2.at[ws, xs], d2s.at[w, xl], d2r.at[ws, xs],
            {"wide": ws, "tp": z * 2 + xs},
        )

    def pair_sum(wp):
        first(wp).wait_recv()
        both = (dkv[wp, r].astype(jnp.float32) + D1[wp].astype(jnp.float32)).astype(low)
        S[wp, 0] = both[:, 0:128]
        S[wp, 1] = both[:, 128:256]

    @pl.loop(0, w + 1)
    def _(i):
        k_rows = kv[0, i]
        v_rows = kv[1, i]
        scores = dot(k_rows, q2[...], NT)
        k_pos = i * 512 + lax.broadcasted_iota(jnp.int32, (512, 1), 0)
        allowed = (k_pos <= q_pos) & (k_pos >= q_start)
        probs = jnp.where(allowed, jnp.exp2(scores * (SCALE * LOG2E) - lse2), 0.0)
        dv = dot(probs.astype(low), g2[...], NN).astype(low)
        prob_grad = dot(v_rows, g2[...], NT)
        ds = (probs * (prob_grad - delta)).astype(low)
        dk = (dot(ds, q2[...], NN) * SCALE).astype(low)
        dq[...] += dot(ds, k_rows, TN)
        for h in range(2):
            dkv[i, h, :, 0:128] = dk[h * QB:(h + 1) * QB, :]
            dkv[i, h, :, 128:256] = dv[h * QB:(h + 1) * QB, :]
        first(i).start()

        @pl.when(i > 0)
        def _():
            pair_sum(i - 1)
            second(i - 1, 0).start()
            second(i - 1, 1).start()

    for h in range(2):
        dqb[:, h * 128:(h + 1) * 128] = (dq[pl.ds(h * QB, QB), :] * SCALE).astype(low)
    QF[r, z, xl] = dqb[...]
    pair_sum(w)
    second(w, 1 - xl).start()

    E = Gather(lambda at, x, row, n: QF.at[r, at, x, pl.ds(row, n), :], ez_s, ez_r, ex_s, ex_r)
    V = Gather(lambda at, x, row, n: KF.at[r, at, x, pl.ds(row, n), :], vz_s, vz_r, vx_s, vx_r)
    E.start()
    load_wq.wait()
    nacc[...] = jnp.zeros_like(nacc)

    E.second()
    out_merge(5)
    out_merge(6)
    out_merge(7)

    def key_sums():
        kacc[...] = S[w, xl].astype(jnp.float32)

        @pl.loop(w + 1, 8)
        def _(ws):
            for xs in range(2):
                arrive(ws, xs).wait_recv()
                kacc[...] += D2[ws, xs].astype(jnp.float32)

        arrive(w, 1 - xl).wait_recv()
        KF[r, z, xl] = (kacc[...] + D2[w, 1 - xl].astype(jnp.float32)).astype(low)

    e_order, e_hands, v_order, v_hands = [], [], [], []

    def pass_on(gather, s, buf, ss, rs, seen, copies):
        gather.whole(s)
        for at in gather.blocks(s):
            k = len(seen)
            c = remote(buf.at[r, at], buf.at[r, at], ss.at[k], rs.at[k], partner)
            c.start()
            seen.append(at)
            copies.append(c)

    def e_whole(s):
        pass_on(E, s, QF, eh_s, eh_r, e_order, e_hands)

    def v_whole(s):
        pass_on(V, s, KF, vh_s, vh_r, v_order, v_hands)

    def process(k):
        at = e_order[k]
        e_hands[k].wait_recv()
        for x in range(2):
            weight = wq[:, aligned(2 * at + x, QB)]
            far = across((2 * at + x) // 3)
            for h in range(2):
                nacc[h] += dot(QF[h, at, x], weight, NT)
            total = dot(N[far, 0:QB, :], QF[0, at, x], TN) + dot(N[far, QB:512, :], QF[1, at, x], TN)
            F[4 * at + 2 * x] = total[:, 0:128].astype(low)
            F[4 * at + 2 * x + 1] = total[:, 128:256].astype(low)

            @pl.when(far == 1)
            def _():
                two_cross(2 * at + x).start()

    def process_kv(k):
        at = v_order[k]
        v_hands[k].wait_recv()
        for x in range(2):
            spot = 32 + 8 * x + at
            weight = wq[:, aligned(spot, 128)]
            far = across(spot // 6)
            for h in range(2):
                nacc[h] += dot(KF[h, at, x], weight, NT)
            total = dot(N[far, 0:QB, :], KF[0, at, x], TN) + dot(N[far, QB:512, :], KF[1, at, x], TN)
            F[spot] = total.astype(low)

            @pl.when(far == 1)
            def _():
                one_cross(spot).start()

    def two_cross(tp):
        ref = pl.ds(2 * tp, 2)
        return remote(F.at[ref], FX.at[ref], f_send.at[2 * tp], fx_recv.at[2 * tp], outer)

    def one_cross(spot):
        return remote(F.at[spot], FX.at[spot], f_send.at[spot], fx_recv.at[spot], outer)

    def two(tp):
        return remote(
            F.at[pl.ds(2 * tp, 2)], FR.at[side, pl.ds(2 * (tp % 3), 2)],
            f_send.at[2 * tp], f_recv.at[side, 2 * (tp % 3)], {"wide": tp // 3},
        )

    def one(spot):
        return remote(
            F.at[spot], FR.at[side, spot % 6], f_send.at[spot], f_recv.at[side, spot % 6],
            {"wide": spot // 6},
        )

    def two_in(sy, j):
        return remote(
            F.at[pl.ds(6 * w + 2 * j, 2)], FR.at[sy, pl.ds(2 * j, 2)],
            f_send.at[6 * w + 2 * j], f_recv.at[sy, 2 * j], {"wide": (w // 4) * 4 + sy},
        )

    def one_in(sy, j):
        return remote(
            F.at[6 * w + j], FR.at[sy, j], f_send.at[6 * w + j], f_recv.at[sy, j],
            {"wide": (w // 4) * 4 + sy},
        )

    def merge(k):
        for x in range(2):
            tp = 2 * e_order[k] + x

            @pl.when(across(tp // 3) == 0)
            def _():
                two_cross(tp).wait_recv()
                for j in range(2):
                    both = F[2 * tp + j].astype(jnp.float32) + FX[2 * tp + j].astype(jnp.float32)
                    F[2 * tp + j] = both.astype(low)

            @pl.when((across(tp // 3) == 0) & (tp // 3 != w))
            def _():
                two(tp).start()

    def merge_kv(k):
        for x in range(2):
            spot = 32 + 8 * x + v_order[k]

            @pl.when(across(spot // 6) == 0)
            def _():
                one_cross(spot).wait_recv()
                F[spot] = (F[spot].astype(jnp.float32) + FX[spot].astype(jnp.float32)).astype(low)

            @pl.when((across(spot // 6) == 0) & (spot // 6 != w))
            def _():
                one(spot).start()

    E.step(1, 0)
    lend_n.wait_recv()
    E.step(1, 1)
    key_sums()
    V.start()
    E.step(1, 2)
    V.second()
    e_whole(0)
    E.step(2, 0)
    E.step(2, 1)
    V.step(1, 0)
    V.step(1, 1)
    process(0)
    E.step(2, 2)
    V.step(1, 2)
    e_whole(1)
    v_whole(0)
    E.step(3, 0)
    process(1)
    merge(0)
    E.step(3, 1)
    V.step(2, 0)
    V.step(2, 1)
    process(2)
    E.step(3, 2)
    V.step(2, 2)
    process_kv(0)
    e_whole(2)
    v_whole(1)
    merge(1)
    E.step(4, 0)
    process(3)
    merge(2)
    E.step(4, 1)
    V.step(3, 0)
    V.step(3, 1)
    process(4)
    merge_kv(0)
    E.step(4, 2)
    V.step(3, 2)
    process_kv(1)
    process_kv(2)
    merge(3)
    e_whole(3)
    v_whole(2)
    process(5)
    process(6)
    merge(4)
    e_whole(4)
    V.step(4, 0)
    V.step(4, 1)
    V.step(4, 2)
    process_kv(3)
    process_kv(4)
    merge_kv(1)
    merge_kv(2)
    process(7)
    merge(5)
    merge(6)
    v_whole(3)
    v_whole(4)
    process_kv(5)
    process_kv(6)
    merge_kv(3)
    merge_kv(4)
    process_kv(7)
    merge(7)
    merge_kv(5)
    merge_kv(6)
    merge_kv(7)

    for h in range(2):
        ng_out[h * QB:(h + 1) * QB, :] = nacc[h].astype(low)

    OR[side] = OP[w]

    @pl.loop(0, 4)
    def _(sy):
        @pl.when(sy != side)
        def _():
            remote(
                OP.at[w], OR.at[sy], o_send.at[w], o_recv.at[sy], {"wide": (w // 4) * 4 + sy}
            ).wait_recv()

    total = OR[0].astype(jnp.float32)
    for sy in range(1, 4):
        total += OR[sy].astype(jnp.float32)
    ow_out[...] = total.astype(low)

    FR[side] = F[pl.ds(6 * w, 6)]

    @pl.loop(0, 4)
    def _(sy):
        @pl.when(sy != side)
        def _():
            for j in range(3):
                @pl.when((w < 5) | ((w == 5) & (j == 0)))
                def _():
                    two_in(sy, j).wait_recv()

            for j in range(6):
                @pl.when((w > 5) | ((w == 5) & (j > 1)))
                def _():
                    one_in(sy, j).wait_recv()

    for j in range(6):
        total = FR[0, j].astype(jnp.float32)
        for sy in range(1, 4):
            total += FR[sy, j].astype(jnp.float32)
        gw_out[:, j * 128:(j + 1) * 128] = total.astype(low)

    for c in sends + pushes + hands + e_hands + v_hands:
        c.wait_send()
    for gather in (A, E, V):
        gather.finish()

    @pl.loop(0, w)
    def _(wp):
        first(wp).wait_send()
        second(wp, 0).wait_send()
        second(wp, 1).wait_send()

    first(w).wait_send()
    second(w, 1 - xl).wait_send()

    @pl.loop(0, 8)
    def _(wp):
        @pl.when(wp != w)
        def _():
            out_chunk(wp).wait_send()

    @pl.loop(0, 16)
    def _(tp):
        @pl.when(tp // 3 != w)
        def _():
            two(tp).wait_send()

        @pl.when((32 + tp) // 6 != w)
        def _():
            one(32 + tp).wait_send()


def emit_kernel(a, b, c, a_out, b_out, c_out, a_in, b_in, c_in, sem):
    loads = [
        pltpu.make_async_copy(x, y, sem.at[0, k])
        for k, (x, y) in enumerate(((a, a_in), (b, b_in), (c, c_in)))
    ]
    stores = [
        pltpu.make_async_copy(x, y, sem.at[1, k])
        for k, (x, y) in enumerate(((a_in, a_out), (b_in, b_out), (c_in, c_out)))
    ]
    for copy in loads:
        copy.start()
    for load, store in zip(loads, stores):
        load.wait()
        store.start()
    for copy in stores:
        copy.wait()


def emit(arrays):
    hbm = pl.BlockSpec(memory_space=pltpu.HBM)
    return pl.pallas_call(
        emit_kernel,
        name="emit",
        out_shape=tuple(jax.ShapeDtypeStruct(a.shape, a.dtype) for a in arrays),
        in_specs=[hbm] * 3,
        out_specs=(hbm,) * 3,
        scratch_shapes=[pltpu.VMEM(a.shape, a.dtype) for a in arrays] + [pltpu.SemaphoreType.DMA((2, 3))],
        compiler_params=pltpu.CompilerParams(vmem_limit_bytes=60 * 1024 * 1024),
        cost_estimate=pl.CostEstimate(flops=1_000_000, bytes_accessed=1_000_000, transcendentals=0),
    )(*arrays)


def local(
    normed, queries, keys, values, attn_out, row_logsumexp, out_grad, out_weight, qkv_weight, documents, tasks
):
    hbm = pl.BlockSpec(memory_space=pltpu.HBM)
    vmem = pl.BlockSpec(memory_space=pltpu.VMEM)
    dma = pltpu.SemaphoreType.DMA
    low, wide = jnp.bfloat16, jnp.float32
    ring = [dma((2, 4, 3)), dma((2, 4, 3)), dma((9,)), dma((9,)), dma((8,)), dma((8,))]
    done = pl.pallas_call(
        whole_kernel,
        name="layer",
        out_shape=(
            jax.ShapeDtypeStruct((512, 128), low),
            jax.ShapeDtypeStruct((QB, QB), low),
            jax.ShapeDtypeStruct((128, 768), low),
        ),
        in_specs=[hbm] * 10,
        out_specs=(vmem, vmem, vmem),
        scratch_shapes=[
            pltpu.VMEM((32, 128), jnp.int32),
            pltpu.VMEM((8, 2, QB, QB), low),
            pltpu.VMEM((8, QB, QB), low),
            pltpu.VMEM((QB, D), low),
            pltpu.VMEM((2, 512, QB), low),
            pltpu.VMEM((8, QB, QB), low),
            pltpu.VMEM((8, QB, QB), low),
            pltpu.VMEM((4, QB, QB), low),
            pltpu.VMEM((QB, QB), wide),
            pltpu.VMEM((2, 8, 512, 128), low),
            pltpu.VMEM((QB, QB), low),
            pltpu.VMEM((2, 4096), wide),
            pltpu.VMEM((512, 128), low),
            pltpu.VMEM((512, 128), low),
            pltpu.VMEM((512, 128), wide),
            pltpu.VMEM((QB, QB), low),
            pltpu.VMEM((8, 2, QB, QB), low),
            pltpu.VMEM((2, 8, 2, QB, QB), low),
            pltpu.VMEM((2, 8, 2, QB, 128), low),
            pltpu.VMEM((8, QB, QB), low),
            pltpu.VMEM((8, 2, QB, 128), low),
            pltpu.VMEM((8, 2, QB, 128), low),
            pltpu.VMEM((48, 128, 128), low),
            pltpu.VMEM((48, 128, 128), low),
            pltpu.VMEM((4, 6, 128, 128), low),
            pltpu.VMEM((2, 512, 128), low),
            pltpu.VMEM((128, 6144), low),
            pltpu.VMEM((2, QB, 128), wide),
            pltpu.VMEM((QB, 128), wide),
            dma((9,)), dma((2,)), dma((7,)), dma((7,)), dma((2,)), dma((2,)), dma((2,)), dma((2,)),
            dma((8,)), dma((8,)), dma((4,)),
        ]
        + ring * 3
        + [dma((8,)), dma((8,)), dma((8, 2)), dma((8, 2)), dma((48,)), dma((48,)), dma((4, 6))],
        compiler_params=pltpu.CompilerParams(
            collective_id=0, has_side_effects=True, vmem_limit_bytes=60 * 1024 * 1024
        ),
        cost_estimate=pl.CostEstimate(
            flops=10_000_000_000, bytes_accessed=40_000_000, transcendentals=2_000_000
        ),
    )(
        normed, queries, keys, values, attn_out, row_logsumexp, out_grad, out_weight, qkv_weight,
        documents.reshape(32, 128),
    )
    return emit(done)


def solution(mesh):
    in_specs = (
        P("wide", ("role", "tp")),
        P("wide", "tp"),
        P("wide", None),
        P("wide", None),
        P("wide", "tp"),
        P("tp", None),
        P("wide", ("role", "tp")),
        P("tp", None),
        P(("role", "tp"), None),
        P(),
        P(),
    )
    out_specs = (P("wide", ("role", "tp")), P("tp", ("role", "wide")), P(("role", "tp"), "wide"))
    return jax.shard_map(local, mesh=mesh, in_specs=in_specs, out_specs=out_specs, check_vma=False)
```

```python
import jax
import jax.numpy as jnp
from jax import lax
from jax.experimental import pallas as pl
from jax.experimental.pallas import tpu as pltpu
from jax.sharding import PartitionSpec as P

MESH = pl.DeviceIdType.MESH
D = 4096
HEAD_SIZE = 128
QB = 256
LOG2E = 1.4426950408889634
SCALE = HEAD_SIZE ** (-0.5)
NT = (((1,), (1,)), ((), ()))
TN = (((0,), (0,)), ((), ()))
NN = (((1,), (0,)), ((), ()))


def dot(a, b, dims):
    return lax.dot_general(a, b, dims, preferred_element_type=jnp.float32)


def aligned(at, size):
    return pl.ds(pl.multiple_of(at * size, size), size)


def remote(src, dst, send, recv, where):
    return pltpu.make_async_remote_copy(
        src_ref=src, dst_ref=dst, send_sem=send, recv_sem=recv, device_id=where, device_id_type=MESH
    )


def greet(places):
    barrier = pltpu.get_barrier_semaphore()
    for where in places:
        pl.semaphore_signal(barrier, inc=1, device_id=where, device_id_type=MESH)
    pl.semaphore_wait(barrier, len(places))


def place():
    r = lax.axis_index("role")
    w = lax.axis_index("wide")
    t = lax.axis_index("tp")
    return r, w, t, t // 2, t % 2


def plane_peer(w, z, xl, k):
    dx, dy = k // 4, k % 4
    peer = ((w // 4 + dx) % 2) * 4 + (w % 4 + dy) % 4
    return {"wide": peer, "tp": z * 2 + (xl if dx == 0 else 1 - xl)}


class Gather:
    def __init__(self, block, zs, zr, xs, xr):
        self.block, self.zs, self.zr, self.xs, self.xr = block, zs, zr, xs, xr
        r, w, t, self.z, self.xl = place()
        self.ways = (
            {"tp": ((self.z + 1) % 8) * 2 + self.xl},
            {"tp": ((self.z + 7) % 8) * 2 + self.xl},
        )
        self.inner = {"tp": self.z * 2 + 1 - self.xl}
        self.sent, self.hops, self.crossed = [], {}, {}

    def at(self, d, s):
        return (self.z + 8 - s) % 8 if d == 0 else (self.z + s) % 8

    def piece(self, at, j, share=None):
        if j < 2:
            return self.block(at, self.xl, 128 * j, 128)
        if share is None:
            return self.block(at, 1 - self.xl, 0, 128)
        return self.block(at, 1 - self.xl, 64 * share, 64)

    def go(self, ref, send, recv, where):
        c = remote(ref, ref, send, recv, where)
        c.start()
        self.sent.append(c)
        return c

    def hop(self, d, s, j):
        ref = self.piece(self.at(d, s), j, d if s == 3 else None)
        self.hops[d, s, j] = self.go(ref, self.zs.at[d, s, j], self.zr.at[d, s, j], self.ways[d])

    def cross(self, at, j, k):
        self.crossed[k] = self.go(self.piece(at, j), self.xs.at[k], self.xr.at[k], self.inner)

    def start(self):
        for j in range(2):
            self.hop(0, 0, j)
            self.hop(1, 0, j)
            self.cross(self.z, j, 8 if j == 0 else 0)

    def second(self):
        self.crossed[8].wait_recv()
        self.hop(0, 0, 2)
        self.hop(1, 0, 2)

    def step(self, s, j):
        for d in range(2):
            if s == 4 and j < 2 and d != j:
                continue
            self.hops[d, s - 1, j].wait_recv()
            if s < 3 or (s == 3 and (j == 2 or d == j)):
                self.hop(d, s, j)
            if j == 1:
                self.cross(self.at(d, s), 1, 7 if s == 4 else 2 * s - 1 + d)

    def whole(self, s):
        for k in ((0,), (1, 2), (3, 4), (5, 6), (7,))[s]:
            self.crossed[k].wait_recv()

    def blocks(self, s):
        return ((self.z + 8 - s) % 8, (self.z + s) % 8) if s in (1, 2, 3) else ((self.z + s) % 8,)

    def finish(self):
        for c in self.sent:
            c.wait_send()


def count_below(docs, value):
    below = jnp.where(docs < value, 1.0, 0.0)
    count = jnp.sum(jnp.sum(below, axis=0, keepdims=True), axis=1, keepdims=True)
    return count.astype(jnp.int32)


def whole_kernel(
    normed, queries, keys, values, ao, lse_in, og, ow, wq_in, docs_in,
    ng_out, ow_out, gw_out,
    docs, G, O, W, AO, OP, OX, OR, acc, kv, Q, lse, q2, g2, dq, dqb, dkv,
    QF, KF, D1, S, D2, F, FX, FR, N, wq, nacc, kacc,
    lsem, swap_sem, k_send, k_recv, kp_sem, ao_sem, aoh_sem, n_sem, o_send, ox_recv, o_recv,
    az_s, az_r, ax_s, ax_r, ah_s, ah_r,
    ez_s, ez_r, ex_s, ex_r, eh_s, eh_r,
    vz_s, vz_r, vx_s, vx_r, vh_s, vh_r,
    d1s, d1r, d2s, d2r, f_send, fx_recv, f_recv,
):
    r, w, t, z, xl = place()
    low = jnp.bfloat16
    partner = {"role": 1 - r}
    inner = {"tp": z * 2 + 1 - xl}
    outer = {"wide": (w + 4) % 8, "tp": z * 2 + 1 - xl}
    side = w % 4
    up = {"tp": ((z + 1) % 8) * 2 + xl}
    down = {"tp": ((z + 7) % 8) * 2 + xl}
    plane = [{"wide": (w + k // 2) % 8, "tp": z * 2 + (xl + k % 2) % 2} for k in range(1, 16)]
    cols = aligned(xl, 128)
    mine = aligned(r, QB)
    other = aligned(1 - r, QB)
    heads = aligned(z, 128)

    @pl.when(r == 0)
    def _():
        pltpu.make_async_copy(keys.at[:, heads], kv.at[r, w], lsem.at[0]).start()

    @pl.when(r == 1)
    def _():
        pltpu.make_async_copy(values.at[:, heads], kv.at[r, w], lsem.at[0]).start()

    load_own = pltpu.make_async_copy(og.at[mine, :], G.at[z, r, :, cols], lsem.at[1])
    load_ao = pltpu.make_async_copy(ao, AO.at[0], lsem.at[2])
    load_w = pltpu.make_async_copy(ow, W, lsem.at[3])
    load_docs = pltpu.make_async_copy(docs_in, docs, lsem.at[4])
    load_q = pltpu.make_async_copy(queries.at[mine, :], Q, lsem.at[5])
    load_lse = pltpu.make_async_copy(lse_in, lse, lsem.at[6])
    load_n = pltpu.make_async_copy(normed, N.at[0], lsem.at[7])
    load_wq = pltpu.make_async_copy(wq_in, wq, lsem.at[8])
    for c in (load_own, load_ao, load_w, load_docs, load_q, load_lse, load_n, load_wq):
        c.start()

    greet([partner, up, down] + plane)

    swap = remote(
        og.at[other, :], G.at[z, r, :, cols], swap_sem.at[0], swap_sem.at[1], partner
    )
    swap.start()
    sends = [swap]
    load_ao.wait()
    lend = remote(AO.at[0, mine], AO.at[1, mine], ao_sem.at[0], ao_sem.at[1], inner)
    lend.start()
    sends.append(lend)
    pltpu.make_async_copy(keys.at[:, heads], kv.at[r, w], lsem.at[0]).wait()
    pushes = []
    for k in range(1, 8):
        c = remote(
            kv.at[r, w], kv.at[r, w], k_send.at[k - 1], k_recv.at[k - 1], plane_peer(w, z, xl, k)
        )
        c.start()
        pushes.append(c)
    load_own.wait()
    swap.wait_recv()

    A = Gather(
        lambda at, x, row, n: G.at[at, :, pl.ds(row, n), aligned(x, 128)], az_s, az_r, ax_s, ax_r
    )
    A.start()
    load_w.wait()
    acc[...] = jnp.zeros_like(acc)
    A.second()

    order, hands = [], []

    def give(at):
        k = len(order)
        c = remote(G.at[at, 1 - r], O.at[at], ah_s.at[k], ah_r.at[k], partner)
        c.start()
        order.append(at)
        hands.append(c)

    def use(at):
        low_cols = aligned(at, QB)
        high_cols = aligned(at + 8, QB)
        acc[...] += dot(G[at, 0], W[:, low_cols], NT) + dot(G[at, 1], W[:, high_cols], NT)

    def across(wp):
        return (wp // 4 + w // 4) % 2

    def out_cross(at):
        return remote(OP.at[at], OX.at[at], o_send.at[at], ox_recv.at[at], outer)

    def out_chunk(at):
        return remote(OP.at[at], OR.at[side], o_send.at[at], o_recv.at[side], {"wide": at})

    def product(k):
        at = order[k]
        far = across(at)
        hands[k].wait_recv()
        total = dot(AO[far, mine, :], G[at, r], TN) + dot(AO[far, other, :], O[at], TN)
        OP[at] = total.astype(low)

        @pl.when(far == 1)
        def _():
            out_cross(at).start()

    def out_merge(k):
        at = order[k]

        @pl.when(across(at) == 0)
        def _():
            out_cross(at).wait_recv()
            OP[at] = (OP[at].astype(jnp.float32) + OX[at].astype(jnp.float32)).astype(low)

        @pl.when((across(at) == 0) & (at != w))
        def _():
            out_chunk(at).start()

    def whole(s):
        A.whole(s)
        for at in A.blocks(s):
            give(at)

    A.step(1, 0)
    A.step(1, 1)
    lend.wait_recv()
    lent = remote(AO.at[1, mine], AO.at[1, mine], aoh_sem.at[0], aoh_sem.at[1], partner)
    lent.start()
    sends.append(lent)
    A.step(1, 2)
    whole(0)
    lent.wait_recv()
    A.step(2, 0)
    A.step(2, 1)
    use(order[0])
    product(0)
    A.step(2, 2)
    whole(1)
    A.step(3, 0)
    use(order[1])
    A.step(3, 1)
    use(order[2])
    product(1)
    A.step(3, 2)
    product(2)
    out_merge(0)
    whole(2)
    A.step(4, 0)
    use(order[3])
    product(3)
    A.step(4, 1)
    use(order[4])
    product(4)
    out_merge(1)
    out_merge(2)
    for c in pushes:
        c.wait_recv()
    hand_kv = remote(kv.at[r], kv.at[r], kp_sem.at[0], kp_sem.at[1], partner)
    hand_kv.start()
    sends.append(hand_kv)
    A.step(4, 2)
    whole(3)
    use(order[5])
    use(order[6])
    whole(4)
    use(order[7])

    load_n.wait()
    lend_n = remote(N.at[0], N.at[1], n_sem.at[0], n_sem.at[1], inner)
    lend_n.start()
    sends.append(lend_n)
    load_docs.wait()
    load_q.wait()
    load_lse.wait()
    start_at = (2 * w + r) * QB
    c1 = count_below(docs[...], 1)
    c2 = count_below(docs[...], 2)
    span = aligned(2 * w + r, QB)
    deltas, lses = [], []
    for h in range(2):
        hc = pl.ds(h * 128, 128)
        q2[pl.ds(h * QB, QB), :] = Q[:, hc]
        g = acc[:, hc].astype(low)
        g2[pl.ds(h * QB, QB), :] = g
        both = g.astype(jnp.float32) * AO[0, mine, hc].astype(jnp.float32)
        deltas.append(jnp.sum(both.T, axis=0, keepdims=True))
        lses.append(lse[pl.ds(h, 1), span] * LOG2E)
    delta = jnp.concatenate(deltas, axis=1)
    lse2 = jnp.concatenate(lses, axis=1)
    lane = lax.broadcasted_iota(jnp.int32, (1, 2 * QB), 1)
    q_pos = start_at + jnp.where(lane >= QB, lane - QB, lane)
    q_start = jnp.where(q_pos >= c2, c2, jnp.where(q_pos >= c1, c1, 0))
    dq[...] = jnp.zeros_like(dq)
    product(5)
    product(6)
    product(7)
    out_merge(3)
    out_merge(4)
    hand_kv.wait_recv()

    def first(wp):
        return remote(dkv.at[wp, 1 - r], D1.at[wp], d1s.at[wp], d1r.at[wp], partner)

    def second(wp, kind):
        return remote(
            S.at[wp, kind], D2.at[w, xl], d2s.at[wp, kind], d2r.at[w, xl],
            {"wide": wp, "tp": z * 2 + kind},
        )

    def arrive(ws, xs):
        return remote(
            S.at[w, xl], D2.at[ws, xs], d2s.at[w, xl], d2r.at[ws, xs],
            {"wide": ws, "tp": z * 2 + xs},
        )

    def pair_sum(wp):
        first(wp).wait_recv()
        both = (dkv[wp, r].astype(jnp.float32) + D1[wp].astype(jnp.float32)).astype(low)
        S[wp, 0] = both[:, 0:128]
        S[wp, 1] = both[:, 128:256]

    def reduce_pair(wp):
        pair_sum(wp)

        @pl.when(wp == w)
        def _():
            second(w, 1 - xl).start()

        @pl.when(wp != w)
        def _():
            second(wp, 0).start()
            second(wp, 1).start()

    @pl.loop(0, w + 1)
    def _(n):
        i = w - n
        k_rows = kv[0, i]
        v_rows = kv[1, i]
        scores = dot(k_rows, q2[...], NT)
        k_pos = i * 512 + lax.broadcasted_iota(jnp.int32, (512, 1), 0)
        allowed = (k_pos <= q_pos) & (k_pos >= q_start)
        probs = jnp.where(allowed, jnp.exp2(scores * (SCALE * LOG2E) - lse2), 0.0)
        dv = dot(probs.astype(low), g2[...], NN).astype(low)
        prob_grad = dot(v_rows, g2[...], NT)
        ds = (probs * (prob_grad - delta)).astype(low)
        dk = (dot(ds, q2[...], NN) * SCALE).astype(low)
        dq[...] += dot(ds, k_rows, TN)
        for h in range(2):
            dkv[i, h, :, 0:128] = dk[h * QB:(h + 1) * QB, :]
            dkv[i, h, :, 128:256] = dv[h * QB:(h + 1) * QB, :]
        first(i).start()

        @pl.when(n > 0)
        def _():
            reduce_pair(i + 1)

    for h in range(2):
        dqb[:, h * 128:(h + 1) * 128] = (dq[pl.ds(h * QB, QB), :] * SCALE).astype(low)
    QF[r, z, xl] = dqb[...]
    reduce_pair(0 * w)

    E = Gather(lambda at, x, row, n: QF.at[r, at, x, pl.ds(row, n), :], ez_s, ez_r, ex_s, ex_r)
    V = Gather(lambda at, x, row, n: KF.at[r, at, x, pl.ds(row, n), :], vz_s, vz_r, vx_s, vx_r)
    E.start()
    load_wq.wait()
    nacc[...] = jnp.zeros_like(nacc)

    E.second()
    out_merge(5)
    out_merge(6)
    out_merge(7)

    def key_sums():
        kacc[...] = S[w, xl].astype(jnp.float32)

        @pl.loop(w + 1, 8)
        def _(ws):
            for xs in range(2):
                arrive(ws, xs).wait_recv()
                kacc[...] += D2[ws, xs].astype(jnp.float32)

        arrive(w, 1 - xl).wait_recv()
        KF[r, z, xl] = (kacc[...] + D2[w, 1 - xl].astype(jnp.float32)).astype(low)

    e_order, e_hands, v_order, v_hands = [], [], [], []

    def pass_on(gather, s, buf, ss, rs, seen, copies):
        gather.whole(s)
        for at in gather.blocks(s):
            k = len(seen)
            c = remote(buf.at[r, at], buf.at[r, at], ss.at[k], rs.at[k], partner)
            c.start()
            seen.append(at)
            copies.append(c)

    def e_whole(s):
        pass_on(E, s, QF, eh_s, eh_r, e_order, e_hands)

    def v_whole(s):
        pass_on(V, s, KF, vh_s, vh_r, v_order, v_hands)

    def process(k):
        at = e_order[k]
        e_hands[k].wait_recv()
        for x in range(2):
            weight = wq[:, aligned(2 * at + x, QB)]
            far = across((2 * at + x) // 3)
            for h in range(2):
                nacc[h] += dot(QF[h, at, x], weight, NT)
            total = dot(N[far, 0:QB, :], QF[0, at, x], TN) + dot(N[far, QB:512, :], QF[1, at, x], TN)
            F[4 * at + 2 * x] = total[:, 0:128].astype(low)
            F[4 * at + 2 * x + 1] = total[:, 128:256].astype(low)

            @pl.when(far == 1)
            def _():
                two_cross(2 * at + x).start()

    def process_kv(k):
        at = v_order[k]
        v_hands[k].wait_recv()
        for x in range(2):
            spot = 32 + 8 * x + at
            weight = wq[:, aligned(spot, 128)]
            far = across(spot // 6)
            for h in range(2):
                nacc[h] += dot(KF[h, at, x], weight, NT)
            total = dot(N[far, 0:QB, :], KF[0, at, x], TN) + dot(N[far, QB:512, :], KF[1, at, x], TN)
            F[spot] = total.astype(low)

            @pl.when(far == 1)
            def _():
                one_cross(spot).start()

    def two_cross(tp):
        ref = pl.ds(2 * tp, 2)
        return remote(F.at[ref], FX.at[ref], f_send.at[2 * tp], fx_recv.at[2 * tp], outer)

    def one_cross(spot):
        return remote(F.at[spot], FX.at[spot], f_send.at[spot], fx_recv.at[spot], outer)

    def two(tp):
        return remote(
            F.at[pl.ds(2 * tp, 2)], FR.at[side, pl.ds(2 * (tp % 3), 2)],
            f_send.at[2 * tp], f_recv.at[side, 2 * (tp % 3)], {"wide": tp // 3},
        )

    def one(spot):
        return remote(
            F.at[spot], FR.at[side, spot % 6], f_send.at[spot], f_recv.at[side, spot % 6],
            {"wide": spot // 6},
        )

    def two_in(sy, j):
        return remote(
            F.at[pl.ds(6 * w + 2 * j, 2)], FR.at[sy, pl.ds(2 * j, 2)],
            f_send.at[6 * w + 2 * j], f_recv.at[sy, 2 * j], {"wide": (w // 4) * 4 + sy},
        )

    def one_in(sy, j):
        return remote(
            F.at[6 * w + j], FR.at[sy, j], f_send.at[6 * w + j], f_recv.at[sy, j],
            {"wide": (w // 4) * 4 + sy},
        )

    def merge(k):
        for x in range(2):
            tp = 2 * e_order[k] + x

            @pl.when(across(tp // 3) == 0)
            def _():
                two_cross(tp).wait_recv()
                for j in range(2):
                    both = F[2 * tp + j].astype(jnp.float32) + FX[2 * tp + j].astype(jnp.float32)
                    F[2 * tp + j] = both.astype(low)

            @pl.when((across(tp // 3) == 0) & (tp // 3 != w))
            def _():
                two(tp).start()

    def merge_kv(k):
        for x in range(2):
            spot = 32 + 8 * x + v_order[k]

            @pl.when(across(spot // 6) == 0)
            def _():
                one_cross(spot).wait_recv()
                F[spot] = (F[spot].astype(jnp.float32) + FX[spot].astype(jnp.float32)).astype(low)

            @pl.when((across(spot // 6) == 0) & (spot // 6 != w))
            def _():
                one(spot).start()

    E.step(1, 0)
    lend_n.wait_recv()
    E.step(1, 1)
    key_sums()
    V.start()
    E.step(1, 2)
    V.second()
    e_whole(0)
    E.step(2, 0)
    E.step(2, 1)
    V.step(1, 0)
    V.step(1, 1)
    process(0)
    E.step(2, 2)
    V.step(1, 2)
    e_whole(1)
    v_whole(0)
    E.step(3, 0)
    process(1)
    merge(0)
    E.step(3, 1)
    V.step(2, 0)
    V.step(2, 1)
    process(2)
    E.step(3, 2)
    V.step(2, 2)
    process_kv(0)
    e_whole(2)
    v_whole(1)
    merge(1)
    E.step(4, 0)
    process(3)
    merge(2)
    E.step(4, 1)
    V.step(3, 0)
    V.step(3, 1)
    process(4)
    merge_kv(0)
    E.step(4, 2)
    V.step(3, 2)
    process_kv(1)
    process_kv(2)
    merge(3)
    e_whole(3)
    v_whole(2)
    process(5)
    process(6)
    merge(4)
    e_whole(4)
    V.step(4, 0)
    V.step(4, 1)
    V.step(4, 2)
    process_kv(3)
    process_kv(4)
    merge_kv(1)
    merge_kv(2)
    process(7)
    merge(5)
    merge(6)
    v_whole(3)
    v_whole(4)
    process_kv(5)
    process_kv(6)
    merge_kv(3)
    merge_kv(4)
    process_kv(7)
    merge(7)
    merge_kv(5)
    merge_kv(6)
    merge_kv(7)

    for h in range(2):
        ng_out[h * QB:(h + 1) * QB, :] = nacc[h].astype(low)

    OR[side] = OP[w]

    @pl.loop(0, 4)
    def _(sy):
        @pl.when(sy != side)
        def _():
            remote(
                OP.at[w], OR.at[sy], o_send.at[w], o_recv.at[sy], {"wide": (w // 4) * 4 + sy}
            ).wait_recv()

    total = OR[0].astype(jnp.float32)
    for sy in range(1, 4):
        total += OR[sy].astype(jnp.float32)
    ow_out[...] = total.astype(low)

    FR[side] = F[pl.ds(6 * w, 6)]

    @pl.loop(0, 4)
    def _(sy):
        @pl.when(sy != side)
        def _():
            for j in range(3):
                @pl.when((w < 5) | ((w == 5) & (j == 0)))
                def _():
                    two_in(sy, j).wait_recv()

            for j in range(6):
                @pl.when((w > 5) | ((w == 5) & (j > 1)))
                def _():
                    one_in(sy, j).wait_recv()

    for j in range(6):
        total = FR[0, j].astype(jnp.float32)
        for sy in range(1, 4):
            total += FR[sy, j].astype(jnp.float32)
        gw_out[:, j * 128:(j + 1) * 128] = total.astype(low)

    for c in sends + pushes + hands + e_hands + v_hands:
        c.wait_send()
    for gather in (A, E, V):
        gather.finish()

    @pl.loop(0, w)
    def _(wp):
        first(wp).wait_send()
        second(wp, 0).wait_send()
        second(wp, 1).wait_send()

    first(w).wait_send()
    second(w, 1 - xl).wait_send()

    @pl.loop(0, 8)
    def _(wp):
        @pl.when(wp != w)
        def _():
            out_chunk(wp).wait_send()

    @pl.loop(0, 16)
    def _(tp):
        @pl.when(tp // 3 != w)
        def _():
            two(tp).wait_send()

        @pl.when((32 + tp) // 6 != w)
        def _():
            one(32 + tp).wait_send()


def emit_kernel(a, b, c, a_out, b_out, c_out, a_in, b_in, c_in, sem):
    loads = [
        pltpu.make_async_copy(x, y, sem.at[0, k])
        for k, (x, y) in enumerate(((a, a_in), (b, b_in), (c, c_in)))
    ]
    stores = [
        pltpu.make_async_copy(x, y, sem.at[1, k])
        for k, (x, y) in enumerate(((a_in, a_out), (b_in, b_out), (c_in, c_out)))
    ]
    for copy in loads:
        copy.start()
    for load, store in zip(loads, stores):
        load.wait()
        store.start()
    for copy in stores:
        copy.wait()


def emit(arrays):
    hbm = pl.BlockSpec(memory_space=pltpu.HBM)
    return pl.pallas_call(
        emit_kernel,
        name="emit",
        out_shape=tuple(jax.ShapeDtypeStruct(a.shape, a.dtype) for a in arrays),
        in_specs=[hbm] * 3,
        out_specs=(hbm,) * 3,
        scratch_shapes=[pltpu.VMEM(a.shape, a.dtype) for a in arrays] + [pltpu.SemaphoreType.DMA((2, 3))],
        compiler_params=pltpu.CompilerParams(vmem_limit_bytes=60 * 1024 * 1024),
        cost_estimate=pl.CostEstimate(flops=1_000_000, bytes_accessed=1_000_000, transcendentals=0),
    )(*arrays)


def local(
    normed, queries, keys, values, attn_out, row_logsumexp, out_grad, out_weight, qkv_weight, documents, tasks
):
    hbm = pl.BlockSpec(memory_space=pltpu.HBM)
    vmem = pl.BlockSpec(memory_space=pltpu.VMEM)
    dma = pltpu.SemaphoreType.DMA
    low, wide = jnp.bfloat16, jnp.float32
    ring = [dma((2, 4, 3)), dma((2, 4, 3)), dma((9,)), dma((9,)), dma((8,)), dma((8,))]
    done = pl.pallas_call(
        whole_kernel,
        name="layer",
        out_shape=(
            jax.ShapeDtypeStruct((512, 128), low),
            jax.ShapeDtypeStruct((QB, QB), low),
            jax.ShapeDtypeStruct((128, 768), low),
        ),
        in_specs=[hbm] * 10,
        out_specs=(vmem, vmem, vmem),
        scratch_shapes=[
            pltpu.VMEM((32, 128), jnp.int32),
            pltpu.VMEM((8, 2, QB, QB), low),
            pltpu.VMEM((8, QB, QB), low),
            pltpu.VMEM((QB, D), low),
            pltpu.VMEM((2, 512, QB), low),
            pltpu.VMEM((8, QB, QB), low),
            pltpu.VMEM((8, QB, QB), low),
            pltpu.VMEM((4, QB, QB), low),
            pltpu.VMEM((QB, QB), wide),
            pltpu.VMEM((2, 8, 512, 128), low),
            pltpu.VMEM((QB, QB), low),
            pltpu.VMEM((2, 4096), wide),
            pltpu.VMEM((512, 128), low),
            pltpu.VMEM((512, 128), low),
            pltpu.VMEM((512, 128), wide),
            pltpu.VMEM((QB, QB), low),
            pltpu.VMEM((8, 2, QB, QB), low),
            pltpu.VMEM((2, 8, 2, QB, QB), low),
            pltpu.VMEM((2, 8, 2, QB, 128), low),
            pltpu.VMEM((8, QB, QB), low),
            pltpu.VMEM((8, 2, QB, 128), low),
            pltpu.VMEM((8, 2, QB, 128), low),
            pltpu.VMEM((48, 128, 128), low),
            pltpu.VMEM((48, 128, 128), low),
            pltpu.VMEM((4, 6, 128, 128), low),
            pltpu.VMEM((2, 512, 128), low),
            pltpu.VMEM((128, 6144), low),
            pltpu.VMEM((2, QB, 128), wide),
            pltpu.VMEM((QB, 128), wide),
            dma((9,)), dma((2,)), dma((7,)), dma((7,)), dma((2,)), dma((2,)), dma((2,)), dma((2,)),
            dma((8,)), dma((8,)), dma((4,)),
        ]
        + ring * 3
        + [dma((8,)), dma((8,)), dma((8, 2)), dma((8, 2)), dma((48,)), dma((48,)), dma((4, 6))],
        compiler_params=pltpu.CompilerParams(
            collective_id=0, has_side_effects=True, vmem_limit_bytes=60 * 1024 * 1024
        ),
        cost_estimate=pl.CostEstimate(
            flops=10_000_000_000, bytes_accessed=40_000_000, transcendentals=2_000_000
        ),
    )(
        normed, queries, keys, values, attn_out, row_logsumexp, out_grad, out_weight, qkv_weight,
        documents.reshape(32, 128),
    )
    return emit(done)


def solution(mesh):
    in_specs = (
        P("wide", ("role", "tp")),
        P("wide", "tp"),
        P("wide", None),
        P("wide", None),
        P("wide", "tp"),
        P("tp", None),
        P("wide", ("role", "tp")),
        P("tp", None),
        P(("role", "tp"), None),
        P(),
        P(),
    )
    out_specs = (P("wide", ("role", "tp")), P("tp", ("role", "wide")), P(("role", "tp"), "wide"))
    return jax.shard_map(local, mesh=mesh, in_specs=in_specs, out_specs=out_specs, check_vma=False)
```

```python
import jax
import jax.numpy as jnp
from jax import lax
from jax.experimental import pallas as pl
from jax.experimental.pallas import tpu as pltpu
from jax.sharding import PartitionSpec as P

MESH = pl.DeviceIdType.MESH
D = 4096
HEAD_SIZE = 128
QB = 256
LOG2E = 1.4426950408889634
SCALE = HEAD_SIZE ** (-0.5)
NT = (((1,), (1,)), ((), ()))
TN = (((0,), (0,)), ((), ()))
NN = (((1,), (0,)), ((), ()))


def dot(a, b, dims):
    return lax.dot_general(a, b, dims, preferred_element_type=jnp.float32)


def aligned(at, size):
    return pl.ds(pl.multiple_of(at * size, size), size)


def remote(src, dst, send, recv, where):
    return pltpu.make_async_remote_copy(
        src_ref=src, dst_ref=dst, send_sem=send, recv_sem=recv, device_id=where, device_id_type=MESH
    )


def greet(places):
    barrier = pltpu.get_barrier_semaphore()
    for where in places:
        pl.semaphore_signal(barrier, inc=1, device_id=where, device_id_type=MESH)
    pl.semaphore_wait(barrier, len(places))


def place():
    r = lax.axis_index("role")
    w = lax.axis_index("wide")
    t = lax.axis_index("tp")
    return r, w, t, t // 2, t % 2


def plane_peer(w, z, xl, k):
    dx, dy = k // 4, k % 4
    peer = ((w // 4 + dx) % 2) * 4 + (w % 4 + dy) % 4
    return {"wide": peer, "tp": z * 2 + (xl if dx == 0 else 1 - xl)}


class Gather:
    def __init__(self, block, zs, zr, xs, xr):
        self.block, self.zs, self.zr, self.xs, self.xr = block, zs, zr, xs, xr
        r, w, t, self.z, self.xl = place()
        self.ways = (
            {"tp": ((self.z + 1) % 8) * 2 + self.xl},
            {"tp": ((self.z + 7) % 8) * 2 + self.xl},
        )
        self.inner = {"tp": self.z * 2 + 1 - self.xl}
        self.sent, self.hops, self.crossed = [], {}, {}

    def at(self, d, s):
        return (self.z + 8 - s) % 8 if d == 0 else (self.z + s) % 8

    def piece(self, at, j, share=None):
        if j < 2:
            return self.block(at, self.xl, 128 * j, 128)
        if share is None:
            return self.block(at, 1 - self.xl, 0, 128)
        return self.block(at, 1 - self.xl, 64 * share, 64)

    def go(self, ref, send, recv, where):
        c = remote(ref, ref, send, recv, where)
        c.start()
        self.sent.append(c)
        return c

    def hop(self, d, s, j):
        ref = self.piece(self.at(d, s), j, d if s == 3 else None)
        self.hops[d, s, j] = self.go(ref, self.zs.at[d, s, j], self.zr.at[d, s, j], self.ways[d])

    def cross(self, at, j, k):
        self.crossed[k] = self.go(self.piece(at, j), self.xs.at[k], self.xr.at[k], self.inner)

    def start(self):
        for j in range(2):
            self.hop(0, 0, j)
            self.hop(1, 0, j)
            self.cross(self.z, j, 8 if j == 0 else 0)

    def second(self):
        self.crossed[8].wait_recv()
        self.hop(0, 0, 2)
        self.hop(1, 0, 2)

    def step(self, s, j):
        for d in range(2):
            if s == 4 and j < 2 and d != j:
                continue
            self.hops[d, s - 1, j].wait_recv()
            if s < 3 or (s == 3 and (j == 2 or d == j)):
                self.hop(d, s, j)
            if j == 1:
                self.cross(self.at(d, s), 1, 7 if s == 4 else 2 * s - 1 + d)

    def whole(self, s):
        for k in ((0,), (1, 2), (3, 4), (5, 6), (7,))[s]:
            self.crossed[k].wait_recv()

    def blocks(self, s):
        return ((self.z + 8 - s) % 8, (self.z + s) % 8) if s in (1, 2, 3) else ((self.z + s) % 8,)

    def finish(self):
        for c in self.sent:
            c.wait_send()


def count_below(docs, value):
    below = jnp.where(docs < value, 1.0, 0.0)
    count = jnp.sum(jnp.sum(below, axis=0, keepdims=True), axis=1, keepdims=True)
    return count.astype(jnp.int32)


def whole_kernel(
    normed, queries, keys, values, ao, lse_in, og, ow, wq_in, docs_in,
    ng_out, ow_out, gw_out,
    docs, G, O, W, AO, OP, OX, OR, acc, kv, Q, lse, q2, g2, dq, dqb, dkv,
    QF, KF, D1, S, D2, F, FX, FR, N, wq, nacc, kacc,
    lsem, swap_sem, k_send, k_recv, kp_sem, ao_sem, aoh_sem, n_sem, o_send, ox_recv, o_recv,
    az_s, az_r, ax_s, ax_r, ah_s, ah_r,
    ez_s, ez_r, ex_s, ex_r, eh_s, eh_r,
    vz_s, vz_r, vx_s, vx_r, vh_s, vh_r,
    d1s, d1r, d2s, d2r, f_send, fx_recv, f_recv,
):
    r, w, t, z, xl = place()
    low = jnp.bfloat16
    partner = {"role": 1 - r}
    inner = {"tp": z * 2 + 1 - xl}
    outer = {"wide": (w + 4) % 8, "tp": z * 2 + 1 - xl}
    side = w % 4
    up = {"tp": ((z + 1) % 8) * 2 + xl}
    down = {"tp": ((z + 7) % 8) * 2 + xl}
    plane = [{"wide": (w + k // 2) % 8, "tp": z * 2 + (xl + k % 2) % 2} for k in range(1, 16)]
    cols = aligned(xl, 128)
    mine = aligned(r, QB)
    other = aligned(1 - r, QB)
    heads = aligned(z, 128)

    @pl.when(r == 0)
    def _():
        pltpu.make_async_copy(keys.at[:, heads], kv.at[r, w], lsem.at[0]).start()

    @pl.when(r == 1)
    def _():
        pltpu.make_async_copy(values.at[:, heads], kv.at[r, w], lsem.at[0]).start()

    load_own = pltpu.make_async_copy(og.at[mine, :], G.at[z, r, :, cols], lsem.at[1])
    load_ao = pltpu.make_async_copy(ao, AO.at[0], lsem.at[2])
    load_w = pltpu.make_async_copy(ow, W, lsem.at[3])
    load_docs = pltpu.make_async_copy(docs_in, docs, lsem.at[4])
    load_q = pltpu.make_async_copy(queries.at[mine, :], Q, lsem.at[5])
    load_lse = pltpu.make_async_copy(lse_in, lse, lsem.at[6])
    load_n = pltpu.make_async_copy(normed, N.at[0], lsem.at[7])
    load_wq = pltpu.make_async_copy(wq_in, wq, lsem.at[8])
    for c in (load_own, load_ao, load_w, load_docs, load_q, load_lse, load_n, load_wq):
        c.start()

    greet([partner, up, down] + plane)

    swap = remote(
        og.at[other, :], G.at[z, r, :, cols], swap_sem.at[0], swap_sem.at[1], partner
    )
    swap.start()
    sends = [swap]
    load_ao.wait()
    lend = remote(AO.at[0, mine], AO.at[1, mine], ao_sem.at[0], ao_sem.at[1], inner)
    lend.start()
    sends.append(lend)
    pltpu.make_async_copy(keys.at[:, heads], kv.at[r, w], lsem.at[0]).wait()
    pushes = []
    for k in range(1, 8):
        c = remote(
            kv.at[r, w], kv.at[r, w], k_send.at[k - 1], k_recv.at[k - 1], plane_peer(w, z, xl, k)
        )
        c.start()
        pushes.append(c)
    load_own.wait()
    swap.wait_recv()

    A = Gather(
        lambda at, x, row, n: G.at[at, :, pl.ds(row, n), aligned(x, 128)], az_s, az_r, ax_s, ax_r
    )
    A.start()
    load_w.wait()
    acc[...] = jnp.zeros_like(acc)
    A.second()

    order, hands = [], []

    def give(at):
        k = len(order)
        c = remote(G.at[at, 1 - r], O.at[at], ah_s.at[k], ah_r.at[k], partner)
        c.start()
        order.append(at)
        hands.append(c)

    def use(at):
        low_cols = aligned(at, QB)
        high_cols = aligned(at + 8, QB)
        acc[...] += dot(G[at, 0], W[:, low_cols], NT) + dot(G[at, 1], W[:, high_cols], NT)

    def across(wp):
        return (wp // 4 + w // 4) % 2

    def out_cross(at):
        return remote(OP.at[at], OX.at[at], o_send.at[at], ox_recv.at[at], outer)

    def out_chunk(at):
        return remote(OP.at[at], OR.at[side], o_send.at[at], o_recv.at[side], {"wide": at})

    def product(k):
        at = order[k]
        far = across(at)
        hands[k].wait_recv()
        total = dot(AO[far, mine, :], G[at, r], TN) + dot(AO[far, other, :], O[at], TN)
        OP[at] = total.astype(low)

        @pl.when(far == 1)
        def _():
            out_cross(at).start()

    def out_merge(k):
        at = order[k]

        @pl.when(across(at) == 0)
        def _():
            out_cross(at).wait_recv()
            OP[at] = (OP[at].astype(jnp.float32) + OX[at].astype(jnp.float32)).astype(low)

        @pl.when((across(at) == 0) & (at != w))
        def _():
            out_chunk(at).start()

    def whole(s):
        A.whole(s)
        for at in A.blocks(s):
            give(at)

    A.step(1, 0)
    A.step(1, 1)
    lend.wait_recv()
    lent = remote(AO.at[1, mine], AO.at[1, mine], aoh_sem.at[0], aoh_sem.at[1], partner)
    lent.start()
    sends.append(lent)
    A.step(1, 2)
    whole(0)
    lent.wait_recv()
    A.step(2, 0)
    A.step(2, 1)
    use(order[0])
    product(0)
    A.step(2, 2)
    whole(1)
    A.step(3, 0)
    use(order[1])
    A.step(3, 1)
    use(order[2])
    product(1)
    A.step(3, 2)
    product(2)
    out_merge(0)
    whole(2)
    A.step(4, 0)
    use(order[3])
    product(3)
    A.step(4, 1)
    use(order[4])
    product(4)
    out_merge(1)
    out_merge(2)
    for c in pushes:
        c.wait_recv()
    hand_kv = remote(kv.at[r], kv.at[r], kp_sem.at[0], kp_sem.at[1], partner)
    hand_kv.start()
    sends.append(hand_kv)
    A.step(4, 2)
    whole(3)
    use(order[5])
    use(order[6])
    whole(4)
    use(order[7])

    load_n.wait()
    lend_n = remote(N.at[0], N.at[1], n_sem.at[0], n_sem.at[1], inner)
    lend_n.start()
    sends.append(lend_n)
    load_docs.wait()
    load_q.wait()
    load_lse.wait()
    start_at = (2 * w + r) * QB
    c1 = count_below(docs[...], 1)
    c2 = count_below(docs[...], 2)
    span = aligned(2 * w + r, QB)
    deltas, lses = [], []
    for h in range(2):
        hc = pl.ds(h * 128, 128)
        q2[pl.ds(h * QB, QB), :] = Q[:, hc]
        g = acc[:, hc].astype(low)
        g2[pl.ds(h * QB, QB), :] = g
        both = g.astype(jnp.float32) * AO[0, mine, hc].astype(jnp.float32)
        deltas.append(jnp.sum(both.T, axis=0, keepdims=True))
        lses.append(lse[pl.ds(h, 1), span] * LOG2E)
    delta = jnp.concatenate(deltas, axis=1)
    lse2 = jnp.concatenate(lses, axis=1)
    lane = lax.broadcasted_iota(jnp.int32, (1, 2 * QB), 1)
    q_pos = start_at + jnp.where(lane >= QB, lane - QB, lane)
    q_start = jnp.where(q_pos >= c2, c2, jnp.where(q_pos >= c1, c1, 0))
    dq[...] = jnp.zeros_like(dq)
    product(5)
    product(6)
    product(7)
    out_merge(3)
    out_merge(4)
    hand_kv.wait_recv()

    def first(wp):
        return remote(dkv.at[wp, 1 - r], D1.at[wp], d1s.at[wp], d1r.at[wp], partner)

    def second(wp, kind):
        return remote(
            S.at[wp, kind], D2.at[w, xl], d2s.at[wp, kind], d2r.at[w, xl],
            {"wide": wp, "tp": z * 2 + kind},
        )

    def arrive(ws, xs):
        return remote(
            S.at[w, xl], D2.at[ws, xs], d2s.at[w, xl], d2r.at[ws, xs],
            {"wide": ws, "tp": z * 2 + xs},
        )

    def pair_sum(wp):
        first(wp).wait_recv()
        both = (dkv[wp, r].astype(jnp.float32) + D1[wp].astype(jnp.float32)).astype(low)
        S[wp, 0] = both[:, 0:128]
        S[wp, 1] = both[:, 128:256]

    def reduce_pair(wp):
        pair_sum(wp)

        @pl.when(wp == w)
        def _():
            second(w, 1 - xl).start()

        @pl.when(wp != w)
        def _():
            second(wp, 0).start()
            second(wp, 1).start()

    @pl.loop(0, w + 1)
    def _(n):
        i = w - n
        k_rows = kv[0, i]
        v_rows = kv[1, i]
        scores = dot(k_rows, q2[...], NT)
        k_pos = i * 512 + lax.broadcasted_iota(jnp.int32, (512, 1), 0)
        allowed = (k_pos <= q_pos) & (k_pos >= q_start)
        probs = jnp.where(allowed, jnp.exp2(scores * (SCALE * LOG2E) - lse2), 0.0)
        dv = dot(probs.astype(low), g2[...], NN).astype(low)
        prob_grad = dot(v_rows, g2[...], NT)
        ds = (probs * (prob_grad - delta)).astype(low)
        dk = (dot(ds, q2[...], NN) * SCALE).astype(low)
        dq[...] += dot(ds, k_rows, TN)
        for h in range(2):
            dkv[i, h, :, 0:128] = dk[h * QB:(h + 1) * QB, :]
            dkv[i, h, :, 128:256] = dv[h * QB:(h + 1) * QB, :]
        first(i).start()

        @pl.when(n > 0)
        def _():
            reduce_pair(i + 1)

    for h in range(2):
        dqb[:, h * 128:(h + 1) * 128] = (dq[pl.ds(h * QB, QB), :] * SCALE).astype(low)
    QF[r, z, xl] = dqb[...]
    reduce_pair(0 * w)

    E = Gather(lambda at, x, row, n: QF.at[r, at, x, pl.ds(row, n), :], ez_s, ez_r, ex_s, ex_r)
    V = Gather(lambda at, x, row, n: KF.at[r, at, x, pl.ds(row, n), :], vz_s, vz_r, vx_s, vx_r)
    E.start()
    load_wq.wait()
    nacc[...] = jnp.zeros_like(nacc)

    E.second()

    def key_sums():
        kacc[...] = S[w, xl].astype(jnp.float32)

        @pl.loop(w + 1, 8)
        def _(ws):
            for xs in range(2):
                arrive(ws, xs).wait_recv()
                kacc[...] += D2[ws, xs].astype(jnp.float32)

        arrive(w, 1 - xl).wait_recv()
        KF[r, z, xl] = (kacc[...] + D2[w, 1 - xl].astype(jnp.float32)).astype(low)

    e_order, e_hands, v_order, v_hands = [], [], [], []

    def pass_on(gather, s, buf, ss, rs, seen, copies):
        gather.whole(s)
        for at in gather.blocks(s):
            k = len(seen)
            c = remote(buf.at[r, at], buf.at[r, at], ss.at[k], rs.at[k], partner)
            c.start()
            seen.append(at)
            copies.append(c)

    def e_whole(s):
        pass_on(E, s, QF, eh_s, eh_r, e_order, e_hands)

    def v_whole(s):
        pass_on(V, s, KF, vh_s, vh_r, v_order, v_hands)

    def process(k):
        at = e_order[k]
        e_hands[k].wait_recv()
        for x in range(2):
            weight = wq[:, aligned(2 * at + x, QB)]
            far = across((2 * at + x) // 3)
            for h in range(2):
                nacc[h] += dot(QF[h, at, x], weight, NT)
            total = dot(N[far, 0:QB, :], QF[0, at, x], TN) + dot(N[far, QB:512, :], QF[1, at, x], TN)
            F[4 * at + 2 * x] = total[:, 0:128].astype(low)
            F[4 * at + 2 * x + 1] = total[:, 128:256].astype(low)

            @pl.when(far == 1)
            def _():
                two_cross(2 * at + x).start()

    def process_kv(k):
        at = v_order[k]
        v_hands[k].wait_recv()
        for x in range(2):
            spot = 32 + 8 * x + at
            weight = wq[:, aligned(spot, 128)]
            far = across(spot // 6)
            for h in range(2):
                nacc[h] += dot(KF[h, at, x], weight, NT)
            total = dot(N[far, 0:QB, :], KF[0, at, x], TN) + dot(N[far, QB:512, :], KF[1, at, x], TN)
            F[spot] = total.astype(low)

            @pl.when(spot // 6 != w)
            def _():
                one(spot).start()

    def two_cross(tp):
        ref = pl.ds(2 * tp, 2)
        return remote(F.at[ref], FX.at[ref], f_send.at[2 * tp], fx_recv.at[2 * tp], outer)

    def two(tp):
        return remote(
            F.at[pl.ds(2 * tp, 2)], FR.at[w, pl.ds(2 * (tp % 3), 2)],
            f_send.at[2 * tp], f_recv.at[w, 2 * (tp % 3)], {"wide": tp // 3},
        )

    def peer(wp):
        return {"wide": wp, "tp": z * 2 + (xl + across(wp)) % 2}

    def one(spot):
        return remote(
            F.at[spot], FR.at[w, spot % 6], f_send.at[spot], f_recv.at[w, spot % 6], peer(spot // 6)
        )

    def two_in(ws, j):
        return remote(
            F.at[pl.ds(6 * w + 2 * j, 2)], FR.at[ws, pl.ds(2 * j, 2)],
            f_send.at[6 * w + 2 * j], f_recv.at[ws, 2 * j], {"wide": ws},
        )

    def one_in(ws, j):
        return remote(F.at[6 * w + j], FR.at[ws, j], f_send.at[6 * w + j], f_recv.at[ws, j], peer(ws))

    for ws in range(8):
        @pl.when((across(ws) == 1) & (w < 6))
        def _():
            FR[ws, 0:2] = jnp.zeros((2, 128, 128), low)

        @pl.when((across(ws) == 1) & (w < 5))
        def _():
            FR[ws, 2:6] = jnp.zeros((4, 128, 128), low)

    def merge(k):
        for x in range(2):
            tp = 2 * e_order[k] + x

            @pl.when(across(tp // 3) == 0)
            def _():
                two_cross(tp).wait_recv()
                for j in range(2):
                    both = F[2 * tp + j].astype(jnp.float32) + FX[2 * tp + j].astype(jnp.float32)
                    F[2 * tp + j] = both.astype(low)

            @pl.when((across(tp // 3) == 0) & (tp // 3 != w))
            def _():
                two(tp).start()

    key_sums()
    V.start()
    E.step(1, 0)
    lend_n.wait_recv()
    E.step(1, 1)
    out_merge(5)
    out_merge(6)
    out_merge(7)
    V.second()
    E.step(1, 2)
    e_whole(0)
    V.step(1, 0)
    E.step(2, 0)
    V.step(1, 1)
    E.step(2, 1)
    process(0)
    E.step(2, 2)
    V.step(1, 2)
    e_whole(1)
    v_whole(0)
    E.step(3, 0)
    process(1)
    merge(0)
    E.step(3, 1)
    V.step(2, 0)
    V.step(2, 1)
    process(2)
    E.step(3, 2)
    V.step(2, 2)
    process_kv(0)
    e_whole(2)
    v_whole(1)
    merge(1)
    E.step(4, 0)
    process(3)
    merge(2)
    E.step(4, 1)
    V.step(3, 0)
    V.step(3, 1)
    process(4)
    E.step(4, 2)
    V.step(3, 2)
    process_kv(1)
    process_kv(2)
    merge(3)
    e_whole(3)
    v_whole(2)
    process(5)
    process(6)
    merge(4)
    e_whole(4)
    V.step(4, 0)
    V.step(4, 1)
    V.step(4, 2)
    process_kv(3)
    process_kv(4)
    process(7)
    merge(5)
    merge(6)
    v_whole(3)
    v_whole(4)
    process_kv(5)
    process_kv(6)
    process_kv(7)
    merge(7)

    for h in range(2):
        ng_out[h * QB:(h + 1) * QB, :] = nacc[h].astype(low)

    OR[side] = OP[w]

    @pl.loop(0, 4)
    def _(sy):
        @pl.when(sy != side)
        def _():
            remote(
                OP.at[w], OR.at[sy], o_send.at[w], o_recv.at[sy], {"wide": (w // 4) * 4 + sy}
            ).wait_recv()

    total = OR[0].astype(jnp.float32)
    for sy in range(1, 4):
        total += OR[sy].astype(jnp.float32)
    ow_out[...] = total.astype(low)

    FR[w] = F[pl.ds(6 * w, 6)]

    @pl.loop(0, 8)
    def _(ws):
        @pl.when(ws != w)
        def _():
            for j in range(3):
                @pl.when((across(ws) == 0) & ((w < 5) | ((w == 5) & (j == 0))))
                def _():
                    two_in(ws, j).wait_recv()

            for j in range(6):
                @pl.when((w > 5) | ((w == 5) & (j > 1)))
                def _():
                    one_in(ws, j).wait_recv()

    for j in range(6):
        total = FR[0, j].astype(jnp.float32)
        for ws in range(1, 8):
            total += FR[ws, j].astype(jnp.float32)
        gw_out[:, j * 128:(j + 1) * 128] = total.astype(low)

    for c in sends + pushes + hands + e_hands + v_hands:
        c.wait_send()
    for gather in (A, E, V):
        gather.finish()

    @pl.loop(0, w)
    def _(wp):
        first(wp).wait_send()
        second(wp, 0).wait_send()
        second(wp, 1).wait_send()

    first(w).wait_send()
    second(w, 1 - xl).wait_send()

    @pl.loop(0, 8)
    def _(wp):
        @pl.when(wp != w)
        def _():
            out_chunk(wp).wait_send()

    @pl.loop(0, 16)
    def _(tp):
        @pl.when(tp // 3 != w)
        def _():
            two(tp).wait_send()

        @pl.when((32 + tp) // 6 != w)
        def _():
            one(32 + tp).wait_send()


def emit_kernel(a, b, c, a_out, b_out, c_out, a_in, b_in, c_in, sem):
    loads = [
        pltpu.make_async_copy(x, y, sem.at[0, k])
        for k, (x, y) in enumerate(((a, a_in), (b, b_in), (c, c_in)))
    ]
    stores = [
        pltpu.make_async_copy(x, y, sem.at[1, k])
        for k, (x, y) in enumerate(((a_in, a_out), (b_in, b_out), (c_in, c_out)))
    ]
    for copy in loads:
        copy.start()
    for load, store in zip(loads, stores):
        load.wait()
        store.start()
    for copy in stores:
        copy.wait()


def emit(arrays):
    hbm = pl.BlockSpec(memory_space=pltpu.HBM)
    return pl.pallas_call(
        emit_kernel,
        name="emit",
        out_shape=tuple(jax.ShapeDtypeStruct(a.shape, a.dtype) for a in arrays),
        in_specs=[hbm] * 3,
        out_specs=(hbm,) * 3,
        scratch_shapes=[pltpu.VMEM(a.shape, a.dtype) for a in arrays] + [pltpu.SemaphoreType.DMA((2, 3))],
        compiler_params=pltpu.CompilerParams(vmem_limit_bytes=60 * 1024 * 1024),
        cost_estimate=pl.CostEstimate(flops=1_000_000, bytes_accessed=1_000_000, transcendentals=0),
    )(*arrays)


def local(
    normed, queries, keys, values, attn_out, row_logsumexp, out_grad, out_weight, qkv_weight, documents, tasks
):
    hbm = pl.BlockSpec(memory_space=pltpu.HBM)
    vmem = pl.BlockSpec(memory_space=pltpu.VMEM)
    dma = pltpu.SemaphoreType.DMA
    low, wide = jnp.bfloat16, jnp.float32
    ring = [dma((2, 4, 3)), dma((2, 4, 3)), dma((9,)), dma((9,)), dma((8,)), dma((8,))]
    done = pl.pallas_call(
        whole_kernel,
        name="layer",
        out_shape=(
            jax.ShapeDtypeStruct((512, 128), low),
            jax.ShapeDtypeStruct((QB, QB), low),
            jax.ShapeDtypeStruct((128, 768), low),
        ),
        in_specs=[hbm] * 10,
        out_specs=(vmem, vmem, vmem),
        scratch_shapes=[
            pltpu.VMEM((32, 128), jnp.int32),
            pltpu.VMEM((8, 2, QB, QB), low),
            pltpu.VMEM((8, QB, QB), low),
            pltpu.VMEM((QB, D), low),
            pltpu.VMEM((2, 512, QB), low),
            pltpu.VMEM((8, QB, QB), low),
            pltpu.VMEM((8, QB, QB), low),
            pltpu.VMEM((4, QB, QB), low),
            pltpu.VMEM((QB, QB), wide),
            pltpu.VMEM((2, 8, 512, 128), low),
            pltpu.VMEM((QB, QB), low),
            pltpu.VMEM((2, 4096), wide),
            pltpu.VMEM((512, 128), low),
            pltpu.VMEM((512, 128), low),
            pltpu.VMEM((512, 128), wide),
            pltpu.VMEM((QB, QB), low),
            pltpu.VMEM((8, 2, QB, QB), low),
            pltpu.VMEM((2, 8, 2, QB, QB), low),
            pltpu.VMEM((2, 8, 2, QB, 128), low),
            pltpu.VMEM((8, QB, QB), low),
            pltpu.VMEM((8, 2, QB, 128), low),
            pltpu.VMEM((8, 2, QB, 128), low),
            pltpu.VMEM((48, 128, 128), low),
            pltpu.VMEM((48, 128, 128), low),
            pltpu.VMEM((8, 6, 128, 128), low),
            pltpu.VMEM((2, 512, 128), low),
            pltpu.VMEM((128, 6144), low),
            pltpu.VMEM((2, QB, 128), wide),
            pltpu.VMEM((QB, 128), wide),
            dma((9,)), dma((2,)), dma((7,)), dma((7,)), dma((2,)), dma((2,)), dma((2,)), dma((2,)),
            dma((8,)), dma((8,)), dma((4,)),
        ]
        + ring * 3
        + [dma((8,)), dma((8,)), dma((8, 2)), dma((8, 2)), dma((48,)), dma((48,)), dma((8, 6))],
        compiler_params=pltpu.CompilerParams(
            collective_id=0, has_side_effects=True, vmem_limit_bytes=60 * 1024 * 1024
        ),
        cost_estimate=pl.CostEstimate(
            flops=10_000_000_000, bytes_accessed=40_000_000, transcendentals=2_000_000
        ),
    )(
        normed, queries, keys, values, attn_out, row_logsumexp, out_grad, out_weight, qkv_weight,
        documents.reshape(32, 128),
    )
    return emit(done)


def solution(mesh):
    in_specs = (
        P("wide", ("role", "tp")),
        P("wide", "tp"),
        P("wide", None),
        P("wide", None),
        P("wide", "tp"),
        P("tp", None),
        P("wide", ("role", "tp")),
        P("tp", None),
        P(("role", "tp"), None),
        P(),
        P(),
    )
    out_specs = (P("wide", ("role", "tp")), P("tp", ("role", "wide")), P(("role", "tp"), "wide"))
    return jax.shard_map(local, mesh=mesh, in_specs=in_specs, out_specs=out_specs, check_vma=False)
```
